128 devices in a mesh: row: 8 (over z, x_lo), col: 16 (over y, x_hi, core).
Axes of the slice: x: 4 (x_hi: 2, x_lo: 2; x = x_hi * 2 + x_lo), y: 4, z: 4, core: 2. Of those that a mesh axis runs over, the one named last changes fastest.
Arguments:
- tokens: bfloat16 [2048, 8192], P('row', 'col'), may hold values from -6 to 6
- gate_frozen_weight: bfloat16 [8192, 28672], P('col', 'row'), may hold values from -0.0625 to 0.0625
- gate_left_factor: bfloat16 [8192, 64], P('col'), may hold values from -0.046875 to 0.046875
- gate_right_factor: bfloat16 [64, 28672], P(None, 'row'), may hold values from -0.75 to 0.75
- gate_column_magnitude: float32 [28672], P('row'), may hold values from 0.5 to 1.5
- up_frozen_weight: bfloat16 [8192, 28672], P('col', 'row'), may hold values from -0.0625 to 0.0625
- up_left_factor: bfloat16 [8192, 64], P('col'), may hold values from -0.046875 to 0.046875
- up_right_factor: bfloat16 [64, 28672], P(None, 'row'), may hold values from -0.75 to 0.75
- up_column_magnitude: float32 [28672], P('row'), may hold values from 0.5 to 1.5
- down_frozen_weight: bfloat16 [28672, 8192], P('row', 'col'), may hold values from -0.03125 to 0.03125
- down_left_factor: bfloat16 [28672, 64], P('row'), may hold values from -0.02734375 to 0.02734375
- down_right_factor: bfloat16 [64, 8192], P(None, 'col'), may hold values from -0.75 to 0.75
- down_column_magnitude: float32 [8192], P('col'), may hold values from 0.5 to 1.5
Outputs:
- mixed: bfloat16 [2048, 8192], P('row', 'col')
The draws below stay inside these ranges and needn't reach their ends.
All inputs are finite; a program needn't handle non-finite values.
Results may differ from the reference program's by a relative error of at most 0.028.
Values may be sent and summed in bfloat16 or wider, within the bound.
A program may use at most 192 MiB of HBM per device.

```python
import jax
import jax.numpy as jnp
from jax import lax

MODEL_WIDTH = 8192
HIDDEN_UNITS = 28672
UPDATE_RANK = 64
TOKENS = 2048
N_ROW = 8
N_COL = 16


def block_levels(own_key, shape, cuts, least, largest):
    def one(axis_at, parts):
        draws = jax.random.uniform(jax.random.fold_in(jax.random.fold_in(own_key, 6), axis_at), (parts,), jnp.float32, least / len(cuts), largest / len(cuts))
        return jnp.repeat(jnp.exp(draws), shape[axis_at] // parts).reshape((-1,) + (1,) * (len(shape) - axis_at - 1))

    loudness = one(*cuts[0])
    for cut in cuts[1:]:
        loudness = loudness * one(*cut)
    return loudness


def normal_values(own_key, shape, deviation, bound, cuts=(), kind=jnp.bfloat16):
    result = deviation * jax.random.normal(own_key, shape, jnp.float32)
    if cuts:
        result = result * block_levels(own_key, shape, cuts, -0.22, 0.18)
    return jnp.clip(result, -bound, bound).astype(kind)


def setup_inputs(seed: int = 0) -> dict:
    keys = jax.random.split(jax.random.key(seed), 14)
    tokens = normal_values(keys[0], (TOKENS, MODEL_WIDTH), 1.0, 6.0, ((0, 8), (1, 16)))
    gate_frozen_weight = normal_values(keys[1], (MODEL_WIDTH, HIDDEN_UNITS), MODEL_WIDTH ** -0.5, 0.0625, ((0, 16), (1, 8)))
    gate_left_factor = normal_values(keys[2], (MODEL_WIDTH, UPDATE_RANK), (0.3 * MODEL_WIDTH ** -0.5), 0.046875, ((0, 16),))
    gate_right_factor = normal_values(keys[3], (UPDATE_RANK, HIDDEN_UNITS), UPDATE_RANK ** -0.5, 0.75, ((1, 8),))
    gate_column_magnitude = jnp.clip(1.0 + 0.1 * jax.random.normal(keys[4], (HIDDEN_UNITS,), jnp.float32), 0.5, 1.5)
    up_frozen_weight = normal_values(keys[5], (MODEL_WIDTH, HIDDEN_UNITS), MODEL_WIDTH ** -0.5, 0.0625, ((0, 16), (1, 8)))
    up_left_factor = normal_values(keys[6], (MODEL_WIDTH, UPDATE_RANK), (0.3 * MODEL_WIDTH ** -0.5), 0.046875, ((0, 16),))
    up_right_factor = normal_values(keys[7], (UPDATE_RANK, HIDDEN_UNITS), UPDATE_RANK ** -0.5, 0.75, ((1, 8),))
    up_column_magnitude = jnp.clip(1.0 + 0.1 * jax.random.normal(keys[8], (HIDDEN_UNITS,), jnp.float32), 0.5, 1.5)
    down_frozen_weight = normal_values(keys[9], (HIDDEN_UNITS, MODEL_WIDTH), HIDDEN_UNITS ** -0.5, 0.03125, ((0, 8), (1, 16)))
    down_left_factor = normal_values(keys[10], (HIDDEN_UNITS, UPDATE_RANK), (0.3 * HIDDEN_UNITS ** -0.5), 0.02734375, ((0, 8),))
    down_right_factor = normal_values(keys[11], (UPDATE_RANK, MODEL_WIDTH), UPDATE_RANK ** -0.5, 0.75, ((1, 16),))
    down_column_magnitude = jnp.clip(1.0 + 0.1 * jax.random.normal(keys[12], (MODEL_WIDTH,), jnp.float32), 0.5, 1.5)
    return dict(tokens=tokens, gate_frozen_weight=gate_frozen_weight, gate_left_factor=gate_left_factor, gate_right_factor=gate_right_factor, gate_column_magnitude=gate_column_magnitude, up_frozen_weight=up_frozen_weight, up_left_factor=up_left_factor, up_right_factor=up_right_factor, up_column_magnitude=up_column_magnitude, down_frozen_weight=down_frozen_weight, down_left_factor=down_left_factor, down_right_factor=down_right_factor, down_column_magnitude=down_column_magnitude)


stability_offset = 1e-06

def column_square_totals(weight, low_b, low_a, blocks):
    height, width = weight.shape
    piece = width // blocks
    weight_blocks = weight.reshape(height, blocks, piece).transpose(1, 0, 2)
    factor_blocks = low_a.reshape(low_a.shape[0], blocks, piece).transpose(1, 0, 2)

    def single(pair):
        merged = pair[0].astype(jnp.float32) + jnp.dot(low_b, pair[1], preferred_element_type=jnp.float32)
        return lax.optimization_barrier(jnp.sum(merged * merged, axis=0))
    return lax.map(single, (weight_blocks, factor_blocks)).reshape(width)

def blocked_direct(inputs, weight, blocks):
    piece = inputs.shape[1] // blocks

    def step(index, total):
        start = (index * piece).astype(jnp.int32)
        left = lax.dynamic_slice_in_dim(inputs, start, piece, 1)
        right = lax.dynamic_slice_in_dim(weight, start, piece, 0)
        rounded = jnp.dot(left, right, preferred_element_type=jnp.float32).astype(jnp.bfloat16)
        rounded = lax.optimization_barrier(rounded)
        return total + rounded.astype(jnp.float32)
    start_total = jnp.zeros((inputs.shape[0], weight.shape[1]), jnp.float32)
    return lax.fori_loop(0, blocks, step, start_total)

def adapted_input(inputs, weight, low_b, low_a, scale):
    direct = blocked_direct(inputs, weight, N_COL)
    coords = jnp.dot(inputs, low_b, preferred_element_type=jnp.float32)
    update = jnp.dot(coords, low_a.astype(jnp.float32), precision=lax.Precision.HIGHEST)
    return (direct + update) * scale[None, :]

def adapted_matrix(inputs, weight, low_b, low_a, scale):
    direct = jnp.dot(inputs, weight, preferred_element_type=jnp.float32)
    coords = jnp.dot(inputs, low_b, preferred_element_type=jnp.float32)
    update = jnp.dot(coords, low_a.astype(jnp.float32), precision=lax.Precision.HIGHEST)
    return (direct + update) * scale[None, :]

def reference(tokens, gate_frozen_weight, gate_left_factor, gate_right_factor, gate_column_magnitude, up_frozen_weight, up_left_factor, up_right_factor, up_column_magnitude, down_frozen_weight, down_left_factor, down_right_factor, down_column_magnitude):
    gate_column_scale = gate_column_magnitude / jnp.sqrt(column_square_totals(gate_frozen_weight, gate_left_factor, gate_right_factor, N_ROW) + stability_offset)
    up_column_scale = up_column_magnitude / jnp.sqrt(column_square_totals(up_frozen_weight, up_left_factor, up_right_factor, N_ROW) + stability_offset)
    down_column_scale = down_column_magnitude / jnp.sqrt(column_square_totals(down_frozen_weight, down_left_factor, down_right_factor, N_COL) + stability_offset)
    gate_preactivation = adapted_input(tokens, gate_frozen_weight, gate_left_factor, gate_right_factor, gate_column_scale)
    up_preactivation = adapted_input(tokens, up_frozen_weight, up_left_factor, up_right_factor, up_column_scale)
    hidden_values = (jax.nn.silu(gate_preactivation) * up_preactivation).astype(jnp.bfloat16)
    mixed = adapted_matrix(hidden_values, down_frozen_weight, down_left_factor, down_right_factor, down_column_scale)
    return mixed.astype(jnp.bfloat16)
```

```python
import functools

import jax
import jax.numpy as jnp
from jax import lax
from jax.experimental import pallas as pl
from jax.experimental.pallas import tpu as pltpu
from jax.sharding import PartitionSpec as P

stability_offset = 1e-06
MESH = pl.DeviceIdType.MESH
NJ = 7


def place():
    r = lax.axis_index("row")
    c = lax.axis_index("col")
    return r // 2, r % 2, c // 4, (c // 2) % 2, c % 2


def device(z, xlo, y, xhi, core):
    return (z * 2 + xlo, (y * 2 + xhi) * 2 + core)


def greet(peers):
    barrier = pltpu.get_barrier_semaphore()
    for peer in peers:
        pl.semaphore_signal(barrier, inc=1, device_id=peer, device_id_type=MESH)
    pl.semaphore_wait(barrier, len(peers))


def send(src, dst, ss, rs, peer):
    return pltpu.make_async_remote_copy(
        src_ref=src, dst_ref=dst, send_sem=ss, recv_sem=rs, device_id=peer, device_id_type=MESH
    )


def column_scale(magnitude, squares):
    return magnitude / jnp.sqrt(squares + stability_offset)


def hidden_kernel(
    tok, gate_w, up_w, left, gate_r, up_r, gate_m, up_m, hid,
    X, W, L, A_s, B_s, C_s, A_r, B_r, C_r, q_s, q_r,
    own, xs, xr, zs, zr, fs, fr, ds, dr, wl, ws, wr, ls, lr, as_, ar, bs, br, cs, cr, qs, qr,
):
    z, xlo, y, xhi, core = place()
    x = xhi * 2 + xlo
    q = xhi * 2 + core
    rb = z * 2 + xlo

    def at_x(d):
        n = (x + d) % 4
        return device(z, n % 2, y, n // 2, core)

    def at_z(d):
        return device((z + d) % 4, xlo, y, xhi, core)

    def at_y(d):
        return device(z, xlo, (y + d) % 4, xhi, core)

    mate = device(z, xlo, y, xhi, 1 - core)
    group = (mate, device(z, xlo, y, 1 - xhi, core), device(z, xlo, y, 1 - xhi, 1 - core))
    group_q = (xhi * 2 + 1 - core, (1 - xhi) * 2 + core, (1 - xhi) * 2 + 1 - core)
    greet((
        at_x(1), at_x(2), at_x(3), at_z(1), at_z(3), mate, group[2], at_y(1), at_y(2), at_y(3),
    ))

    def tile(dz, d, lo=0, n=256):
        xt = (x + 4 - d) % 4
        zt = (z + dz) % 4
        lane = pl.multiple_of(((xt // 2) * 2 + core) * 512, 512)
        return X.at[zt * 2 + xt % 2, pl.ds(lo, n), pl.ds(lane, 512)]

    mine = tile(0, 0)
    started = []

    def go(copy):
        copy.start()
        started.append(copy)
        return copy

    x_in = [None] * 4
    for d in (1, 3, 2):
        x_in[d] = go(send(tok, mine, xs.at[d - 1], xr.at[d - 1], at_x(d)))
    z_in = [[None] * 4, [None] * 4]
    z_in[0][0] = go(send(tok, mine, zs.at[0, 0], zr.at[0, 0], at_z(1)))
    z_in[1][0] = go(send(tok, mine, zs.at[1, 0], zr.at[1, 0], at_z(3)))
    d_in = [[None] * 4 for _ in range(4)]
    d_in[0][0] = go(send(tok, mine, ds.at[0, 0], dr.at[0, 0], mate))
    keep = pltpu.make_async_copy(tok, mine, own.at[0])
    keep.start()

    rows = pl.ds(pl.multiple_of(q * 512, 512), 512)
    l_in = [go(send(left, L.at[rows], ls.at[t], lr.at[t], group[t])) for t in range(3)]
    keep_l = pltpu.make_async_copy(left, L.at[rows], own.at[1])
    keep_l.start()

    def weight_copies(j):
        local, remote = [], []
        for g, w in enumerate((gate_w, up_w)):
            dst = W.at[j, rows, pl.ds(g * 128, 128)]
            for t in (1, 2, 0):
                cols = pl.ds(pl.multiple_of(group_q[t] * 896 + j * 128, 128), 128)
                remote.append(send(w.at[:, cols], dst, ws.at[j, g, t], wr.at[j, g, t], group[t]))
            cols = pl.ds(pl.multiple_of(q * 896 + j * 128, 128), 128)
            local.append(pltpu.make_async_copy(w.at[:, cols], dst, wl.at[j, g]))
        return local, remote

    def fetch(j):
        local, remote = weight_copies(j)
        for copy in remote + local:
            copy.start()

    fetch(0)

    for d in (1, 3, 2):
        x_in[d].wait_recv()
        here = tile(0, d)
        z_in[0][d] = go(send(here, here, zs.at[0, d], zr.at[0, d], at_z(1)))
        z_in[1][d] = go(send(here, here, zs.at[1, d], zr.at[1, d], at_z(3)))
        d_in[0][d] = go(send(here, here, ds.at[0, d], dr.at[0, d], mate))
    fetch(1)
    f_in = [[None] * 4, [None] * 4]
    for d in (0, 1, 3, 2):
        for s in range(2):
            z_in[s][d].wait_recv()
            dz = 3 if s == 0 else 1
            part = tile(dz, d, 128 * s, 128)
            f_in[s][d] = go(send(part, part, fs.at[s, d], fr.at[s, d], at_z(1 if s == 0 else 3)))
            here = tile(dz, d)
            d_in[1 + s][d] = go(send(here, here, ds.at[1 + s, d], dr.at[1 + s, d], mate))
        if d in (0, 1, 3):
            fetch((2, 3, None, 4)[d])
    for d in (0, 1, 3, 2):
        f_in[0][d].wait_recv()
        f_in[1][d].wait_recv()
        here = tile(2, d)
        d_in[3][d] = go(send(here, here, ds.at[3, d], dr.at[3, d], mate))
    keep.wait()
    keep_l.wait()
    for copy in l_in:
        copy.wait_recv()
    for i in range(4):
        for d in range(4):
            d_in[i][d].wait_recv()

    def partial(b, h, j):
        t = X[pl.ds(4 * h, 4), pl.ds(pl.multiple_of(b * 64, 64), 64), :].reshape(256, 2048)
        return jnp.dot(t, W[j], preferred_element_type=jnp.float32)

    def chain(j, h):
        return send(A_s.at[j, h], A_r.at[j, h], as_.at[j, h], ar.at[j, h], at_y(1 if h == 0 else 3))

    def direct(j, h):
        return send(B_s.at[j, h], B_r.at[j, h], bs.at[j, h], br.at[j, h], at_y(3 if h == 0 else 1))

    def last(j, h):
        return send(C_s.at[j, h], C_r.at[j, h], cs.at[j, h], cr.at[j, h], at_y(1 if h == 0 else 3))

    def squares(j):
        return [send(q_s.at[j], q_r.at[j, d - 1], qs.at[j, d - 1], qr.at[j, d - 1], at_y(d)) for d in (1, 2, 3)]

    def finish(j):
        for copy in squares(j):
            copy.wait_recv()
        sq = jnp.sum(q_s[j] + q_r[j, 0] + q_r[j, 1] + q_r[j, 2], axis=0, keepdims=True)
        cols = pl.ds(pl.multiple_of(q * 896 + j * 128, 128), 128)
        gate_scale = column_scale(gate_m[:, cols], sq[:, :128])
        up_scale = column_scale(up_m[:, cols], sq[:, 128:])
        for h in range(2):
            direct(j, h).wait_recv()
            last(j, h).wait_recv()
            total = partial(y, h, j) + B_r[j, h].astype(jnp.float32) + C_r[j, h].astype(jnp.float32)
            gate = total[:, :128] * gate_scale
            up = total[:, 128:] * up_scale
            value = gate / (1.0 + jnp.exp(-gate)) * up
            hid[pl.ds(4 * h, 4), :, pl.ds(pl.multiple_of(j * 128, 128), 128)] = value.astype(
                jnp.bfloat16
            ).reshape(4, 64, 128)

    @pl.loop(0, NJ)
    def _(j):
        @pl.when(j < NJ - 5)
        def _():
            fetch(j + 5)

        local, remote = weight_copies(j)
        for copy in local:
            copy.wait()
        for copy in remote:
            copy.wait_recv()
        cols = pl.ds(pl.multiple_of(q * 896 + j * 128, 128), 128)
        zero = jnp.zeros((64, 128), jnp.bfloat16)
        right = jnp.concatenate(
            [
                jnp.concatenate([gate_r[:, cols], zero], axis=1),
                jnp.concatenate([zero, up_r[:, cols]], axis=1),
            ],
            axis=0,
        )
        q_s[j] = jnp.zeros((8, 256), jnp.float32)

        @pl.loop(0, 8)
        def _(i):
            part = pl.ds(pl.multiple_of(i * 256, 256), 256)
            merged = W[j, part].astype(jnp.float32) + jnp.dot(
                L[part], right, preferred_element_type=jnp.float32
            )
            q_s[j] += jnp.sum((merged * merged).reshape(32, 8, 256), axis=0)
            W[j, part] = merged.astype(jnp.bfloat16)

        for h in range(2):
            A_s[j, h] = partial((y + 2) % 4, h, j).astype(jnp.bfloat16)
            chain(j, h).start()
        for copy in squares(j):
            copy.start()
        for h in range(2):
            B_s[j, h] = partial((y + (3 if h == 0 else 1)) % 4, h, j).astype(jnp.bfloat16)
            direct(j, h).start()
        for h in range(2):
            value = partial((y + (1 if h == 0 else 3)) % 4, h, j)
            chain(j, h).wait_recv()
            C_s[j, h] = (value + A_r[j, h].astype(jnp.float32)).astype(jnp.bfloat16)
            last(j, h).start()

        @pl.when(j >= 1)
        def _():
            finish(j - 1)

    finish(NJ - 1)

    for copy in started:
        copy.wait_send()

    @pl.loop(0, NJ)
    def _(j):
        for copy in weight_copies(j)[1] + squares(j):
            copy.wait_send()
        for h in range(2):
            chain(j, h).wait_send()
            direct(j, h).wait_send()
            last(j, h).wait_send()


def hidden_of(tok, gate_w, up_w, left, gate_r, up_r, gate_m, up_m):
    anywhere = pl.BlockSpec(memory_space=pl.ANY)
    vmem = pl.BlockSpec(memory_space=pltpu.VMEM)
    dma = lambda *s: pltpu.SemaphoreType.DMA(s)
    piece = lambda: pltpu.VMEM((NJ, 2, 256, 256), jnp.bfloat16)
    return pl.pallas_call(
        hidden_kernel,
        out_shape=jax.ShapeDtypeStruct((8, 64, 896), jnp.bfloat16),
        in_specs=[anywhere, anywhere, anywhere, vmem, vmem, vmem, vmem, vmem],
        out_specs=vmem,
        scratch_shapes=[
            pltpu.VMEM((8, 256, 2048), jnp.bfloat16),
            pltpu.VMEM((NJ, 2048, 256), jnp.bfloat16),
            pltpu.VMEM((2048, 128), jnp.bfloat16),
            piece(), piece(), piece(), piece(), piece(), piece(),
            pltpu.VMEM((NJ, 8, 256), jnp.float32),
            pltpu.VMEM((NJ, 3, 8, 256), jnp.float32),
            dma(2), dma(3), dma(3), dma(2, 4), dma(2, 4), dma(2, 4), dma(2, 4), dma(4, 4), dma(4, 4),
            dma(NJ, 2), dma(NJ, 2, 3), dma(NJ, 2, 3), dma(3), dma(3),
            dma(NJ, 2), dma(NJ, 2), dma(NJ, 2), dma(NJ, 2), dma(NJ, 2), dma(NJ, 2),
            dma(NJ, 3), dma(NJ, 3),
        ],
        compiler_params=pltpu.CompilerParams(
            collective_id=0, has_side_effects=True, vmem_limit_bytes=60 * 2**20
        ),
        name="hidden_kernel",
    )(tok, gate_w, up_w, left, gate_r, up_r, gate_m, up_m)


def shards(
    tokens,
    gate_frozen_weight, gate_left_factor, gate_right_factor, gate_column_magnitude,
    up_frozen_weight, up_left_factor, up_right_factor, up_column_magnitude,
    down_frozen_weight, down_left_factor, down_right_factor, down_column_magnitude,
):
    left = jnp.concatenate([gate_left_factor, up_left_factor], axis=1)
    hidden = hidden_of(
        tokens, gate_frozen_weight, up_frozen_weight, left, gate_right_factor, up_right_factor,
        gate_column_magnitude[None], up_column_magnitude[None],
    )
    merged = down_frozen_weight.astype(jnp.float32) + jnp.dot(
        down_left_factor, down_right_factor, preferred_element_type=jnp.float32
    )
    squares = jnp.sum(merged * merged, axis=0)
    squares = lax.psum(squares, "row")
    scale = column_scale(down_column_magnitude, squares)
    full = lax.all_gather(hidden, "col", axis=0, tiled=False)
    full = full.reshape(4, 4, 8, 64, 896).transpose(2, 0, 3, 1, 4).reshape(2048, 3584)
    out = jnp.dot(full, merged.astype(jnp.bfloat16), preferred_element_type=jnp.float32)
    tiles = lax.all_to_all(out.astype(jnp.bfloat16).reshape(8, 256, 512), "row", 0, 0, tiled=True)
    mixed = jnp.sum(tiles.astype(jnp.float32), axis=0)
    return (mixed * scale[None, :]).astype(jnp.bfloat16)


def solution(mesh):
    placed = (
        P("row", "col"),
        P("col", "row"), P("col", None), P(None, "row"), P("row"),
        P("col", "row"), P("col", None), P(None, "row"), P("row"),
        P("row", "col"), P("row", None), P(None, "col"), P("col"),
    )
    return jax.shard_map(
        shards, mesh=mesh, in_specs=placed, out_specs=P("row", "col"), check_vma=False
    )
```

```python
import functools

import jax
import jax.numpy as jnp
from jax import lax
from jax.experimental import pallas as pl
from jax.experimental.pallas import tpu as pltpu
from jax.sharding import PartitionSpec as P

stability_offset = 1e-06
MESH = pl.DeviceIdType.MESH
NJ = 7


def place():
    r = lax.axis_index("row")
    c = lax.axis_index("col")
    return r // 2, r % 2, c // 4, (c // 2) % 2, c % 2


def device(z, xlo, y, xhi, core):
    return (z * 2 + xlo, (y * 2 + xhi) * 2 + core)


def greet(peers):
    barrier = pltpu.get_barrier_semaphore()
    for peer in peers:
        pl.semaphore_signal(barrier, inc=1, device_id=peer, device_id_type=MESH)
    pl.semaphore_wait(barrier, len(peers))


def send(src, dst, ss, rs, peer):
    return pltpu.make_async_remote_copy(
        src_ref=src, dst_ref=dst, send_sem=ss, recv_sem=rs, device_id=peer, device_id_type=MESH
    )


def column_scale(magnitude, squares):
    return magnitude / jnp.sqrt(squares + stability_offset)


def hidden_kernel(
    tok, gate_w, up_w, left, gate_r, up_r, gate_m, up_m, hid,
    X, W, L, A_s, B_s, C_s, A_r, B_r, C_r, q_s, q_r,
    own, xs, xr, zs, zr, fs, fr, ds, dr, wl, ws, wr, ls, lr, as_, ar, bs, br, cs, cr, qs, qr,
):
    z, xlo, y, xhi, core = place()
    x = xhi * 2 + xlo
    q = xhi * 2 + core
    rb = z * 2 + xlo

    def at_x(d):
        n = (x + d) % 4
        return device(z, n % 2, y, n // 2, core)

    def at_z(d):
        return device((z + d) % 4, xlo, y, xhi, core)

    def at_y(d):
        return device(z, xlo, (y + d) % 4, xhi, core)

    mate = device(z, xlo, y, xhi, 1 - core)
    group = (mate, device(z, xlo, y, 1 - xhi, core), device(z, xlo, y, 1 - xhi, 1 - core))
    group_q = (xhi * 2 + 1 - core, (1 - xhi) * 2 + core, (1 - xhi) * 2 + 1 - core)
    greet((
        at_x(1), at_x(2), at_x(3), at_z(1), at_z(3), mate, group[2], at_y(1), at_y(2), at_y(3),
    ))

    def tile(dz, d, lo=0, n=256):
        xt = (x + 4 - d) % 4
        zt = (z + dz) % 4
        lane = pl.multiple_of(((xt // 2) * 2 + core) * 512, 512)
        return X.at[zt * 2 + xt % 2, pl.ds(lo, n), pl.ds(lane, 512)]

    mine = tile(0, 0)
    started = []

    def go(copy):
        copy.start()
        started.append(copy)
        return copy

    x_in = [None] * 4
    for d in (1, 3, 2):
        x_in[d] = go(send(tok, mine, xs.at[d - 1], xr.at[d - 1], at_x(d)))
    z_in = [[None] * 4, [None] * 4]
    z_in[0][0] = go(send(tok, mine, zs.at[0, 0], zr.at[0, 0], at_z(1)))
    z_in[1][0] = go(send(tok, mine, zs.at[1, 0], zr.at[1, 0], at_z(3)))
    d_in = [[None] * 4 for _ in range(4)]
    d_in[0][0] = go(send(tok, mine, ds.at[0, 0], dr.at[0, 0], mate))
    keep = pltpu.make_async_copy(tok, mine, own.at[0])
    keep.start()

    rows = pl.ds(pl.multiple_of(q * 512, 512), 512)
    l_in = [go(send(left, L.at[rows], ls.at[t], lr.at[t], group[t])) for t in range(3)]
    keep_l = pltpu.make_async_copy(left, L.at[rows], own.at[1])
    keep_l.start()

    def weight_copies(j):
        local, remote = [], []
        for g, w in enumerate((gate_w, up_w)):
            dst = W.at[j, rows, pl.ds(g * 128, 128)]
            for t in (1, 2, 0):
                cols = pl.ds(pl.multiple_of(group_q[t] * 896 + j * 128, 128), 128)
                remote.append(send(w.at[:, cols], dst, ws.at[j, g, t], wr.at[j, g, t], group[t]))
            cols = pl.ds(pl.multiple_of(q * 896 + j * 128, 128), 128)
            local.append(pltpu.make_async_copy(w.at[:, cols], dst, wl.at[j, g]))
        return local, remote

    def fetch(j):
        local, remote = weight_copies(j)
        for copy in remote + local:
            copy.start()

    fetch(0)

    for d in (1, 3, 2):
        x_in[d].wait_recv()
        here = tile(0, d)
        z_in[0][d] = go(send(here, here, zs.at[0, d], zr.at[0, d], at_z(1)))
        z_in[1][d] = go(send(here, here, zs.at[1, d], zr.at[1, d], at_z(3)))
        d_in[0][d] = go(send(here, here, ds.at[0, d], dr.at[0, d], mate))
    fetch(1)
    f_in = [[None] * 4, [None] * 4]
    for d in (0, 1, 3, 2):
        for s in range(2):
            z_in[s][d].wait_recv()
            dz = 3 if s == 0 else 1
            part = tile(dz, d, 128 * s, 128)
            f_in[s][d] = go(send(part, part, fs.at[s, d], fr.at[s, d], at_z(1 if s == 0 else 3)))
            here = tile(dz, d)
            d_in[1 + s][d] = go(send(here, here, ds.at[1 + s, d], dr.at[1 + s, d], mate))
        if d in (0, 1, 3):
            fetch((2, 3, None, 4)[d])
    for d in (0, 1, 3, 2):
        f_in[0][d].wait_recv()
        f_in[1][d].wait_recv()
        here = tile(2, d)
        d_in[3][d] = go(send(here, here, ds.at[3, d], dr.at[3, d], mate))
    keep.wait()
    keep_l.wait()
    for copy in l_in:
        copy.wait_recv()
    for i in range(4):
        for d in range(4):
            d_in[i][d].wait_recv()

    def partial(b, h, j):
        t = X[pl.ds(4 * h, 4), pl.ds(pl.multiple_of(b * 64, 64), 64), :].reshape(256, 2048)
        return jnp.dot(t, W[j], preferred_element_type=jnp.float32)

    def chain(j, h):
        return send(A_s.at[j, h], A_r.at[j, h], as_.at[j, h], ar.at[j, h], at_y(1 if h == 0 else 3))

    def direct(j, h):
        return send(B_s.at[j, h], B_r.at[j, h], bs.at[j, h], br.at[j, h], at_y(3 if h == 0 else 1))

    def last(j, h):
        return send(C_s.at[j, h], C_r.at[j, h], cs.at[j, h], cr.at[j, h], at_y(1 if h == 0 else 3))

    def squares(j):
        return [send(q_s.at[j], q_r.at[j, d - 1], qs.at[j, d - 1], qr.at[j, d - 1], at_y(d)) for d in (1, 2, 3)]

    def finish(j):
        for copy in squares(j):
            copy.wait_recv()
        sq = jnp.sum(q_s[j] + q_r[j, 0] + q_r[j, 1] + q_r[j, 2], axis=0, keepdims=True)
        cols = pl.ds(pl.multiple_of(q * 896 + j * 128, 128), 128)
        gate_scale = column_scale(gate_m[:, cols], sq[:, :128])
        up_scale = column_scale(up_m[:, cols], sq[:, 128:])
        for h in range(2):
            direct(j, h).wait_recv()
            last(j, h).wait_recv()
            total = partial(y, h, j) + B_r[j, h].astype(jnp.float32) + C_r[j, h].astype(jnp.float32)
            gate = total[:, :128] * gate_scale
            up = total[:, 128:] * up_scale
            value = gate / (1.0 + jnp.exp(-gate)) * up
            hid[pl.ds(4 * h, 4), :, pl.ds(pl.multiple_of(j * 128, 128), 128)] = value.astype(
                jnp.bfloat16
            ).reshape(4, 64, 128)

    @pl.loop(0, NJ)
    def _(j):
        @pl.when(j < NJ - 5)
        def _():
            fetch(j + 5)

        local, remote = weight_copies(j)
        for copy in local:
            copy.wait()
        for copy in remote:
            copy.wait_recv()
        cols = pl.ds(pl.multiple_of(q * 896 + j * 128, 128), 128)
        zero = jnp.zeros((64, 128), jnp.bfloat16)
        right = jnp.concatenate(
            [
                jnp.concatenate([gate_r[:, cols], zero], axis=1),
                jnp.concatenate([zero, up_r[:, cols]], axis=1),
            ],
            axis=0,
        )
        q_s[j] = jnp.zeros((8, 256), jnp.float32)

        @pl.loop(0, 8)
        def _(i):
            part = pl.ds(pl.multiple_of(i * 256, 256), 256)
            merged = W[j, part].astype(jnp.float32) + jnp.dot(
                L[part], right, preferred_element_type=jnp.float32
            )
            q_s[j] += jnp.sum((merged * merged).reshape(32, 8, 256), axis=0)
            W[j, part] = merged.astype(jnp.bfloat16)

        for h in range(2):
            A_s[j, h] = partial((y + 2) % 4, h, j).astype(jnp.bfloat16)
            chain(j, h).start()
        for copy in squares(j):
            copy.start()
        for h in range(2):
            B_s[j, h] = partial((y + (3 if h == 0 else 1)) % 4, h, j).astype(jnp.bfloat16)
            direct(j, h).start()
        for h in range(2):
            value = partial((y + (1 if h == 0 else 3)) % 4, h, j)
            chain(j, h).wait_recv()
            C_s[j, h] = (value + A_r[j, h].astype(jnp.float32)).astype(jnp.bfloat16)
            last(j, h).start()

        @pl.when(j >= 1)
        def _():
            finish(j - 1)

    finish(NJ - 1)

    for copy in started:
        copy.wait_send()

    @pl.loop(0, NJ)
    def _(j):
        for copy in weight_copies(j)[1] + squares(j):
            copy.wait_send()
        for h in range(2):
            chain(j, h).wait_send()
            direct(j, h).wait_send()
            last(j, h).wait_send()


def hidden_of(tok, gate_w, up_w, left, gate_r, up_r, gate_m, up_m):
    anywhere = pl.BlockSpec(memory_space=pl.ANY)
    vmem = pl.BlockSpec(memory_space=pltpu.VMEM)
    dma = lambda *s: pltpu.SemaphoreType.DMA(s)
    piece = lambda: pltpu.VMEM((NJ, 2, 256, 256), jnp.bfloat16)
    return pl.pallas_call(
        hidden_kernel,
        out_shape=jax.ShapeDtypeStruct((8, 64, 896), jnp.bfloat16),
        in_specs=[anywhere, anywhere, anywhere, vmem, vmem, vmem, vmem, vmem],
        out_specs=vmem,
        scratch_shapes=[
            pltpu.VMEM((8, 256, 2048), jnp.bfloat16),
            pltpu.VMEM((NJ, 2048, 256), jnp.bfloat16),
            pltpu.VMEM((2048, 128), jnp.bfloat16),
            piece(), piece(), piece(), piece(), piece(), piece(),
            pltpu.VMEM((NJ, 8, 256), jnp.float32),
            pltpu.VMEM((NJ, 3, 8, 256), jnp.float32),
            dma(2), dma(3), dma(3), dma(2, 4), dma(2, 4), dma(2, 4), dma(2, 4), dma(4, 4), dma(4, 4),
            dma(NJ, 2), dma(NJ, 2, 3), dma(NJ, 2, 3), dma(3), dma(3),
            dma(NJ, 2), dma(NJ, 2), dma(NJ, 2), dma(NJ, 2), dma(NJ, 2), dma(NJ, 2),
            dma(NJ, 3), dma(NJ, 3),
        ],
        compiler_params=pltpu.CompilerParams(
            collective_id=0, has_side_effects=True, vmem_limit_bytes=60 * 2**20
        ),
        name="hidden_kernel",
    )(tok, gate_w, up_w, left, gate_r, up_r, gate_m, up_m)


def mix_kernel(
    hid, down_w, left, right, mag, out,
    H, W, R, M_s, M_r, F, G, A_s, B_s, C_s, A_r, B_r, C_r, D_s, D_r, sq, q_m, q_t, q_r,
    own, hs, hr, ys, yr, fs, fr, ws, wr, ms, mr, as_, ar, bs, br, cs, cr, ds, dr, qs, qr,
):
    z, xlo, y, xhi, core = place()

    def at(dz=0, dx=0, dy=0):
        return device((z + dz) % 4, (xlo + dx) % 2, (y + dy) % 4, xhi, core)

    mate = device(z, xlo, y, xhi, 1 - core)
    across = device(z, xlo, y, 1 - xhi, core)
    rows_peers = [(dz, dx) for dz in range(4) for dx in range(2)][1:]
    greet([mate, across, at(dy=1), at(dy=3)] + [at(dz=dz, dx=dx) for dz, dx in rows_peers])
    started = []

    def go(copy):
        copy.start()
        started.append(copy)
        return copy

    h_in = go(send(hid, H.at[y, xhi], hs.at[0], hr.at[0], across))
    y_in = [[None, None], [None, None]]
    for s in range(2):
        y_in[s][0] = go(send(hid, H.at[y, xhi], ys.at[s, 0], yr.at[s, 0], at(dy=1 if s == 0 else 3)))
    keep = pltpu.make_async_copy(hid, H.at[y, xhi], own.at[0])
    keep.start()

    w_in, w_own = [], []
    w_in.append(go(send(right, R.at[core], ws.at[2], wr.at[2], mate)))
    for xh in range(2):
        theirs = pl.ds(pl.multiple_of((xh * 2 + 1 - core) * 896, 128), 896)
        ours = pl.ds(pl.multiple_of((xh * 2 + core) * 896, 128), 896)
        w_in.append(go(send(down_w.at[theirs], W.at[core, xh], ws.at[xh], wr.at[xh], mate)))
        w_own.append(pltpu.make_async_copy(down_w.at[ours], W.at[core, xh], own.at[1 + xh]))
    w_own.append(pltpu.make_async_copy(right, R.at[core], own.at[3]))
    for copy in w_own:
        copy.start()
    for copy in w_own:
        copy.wait()
    for copy in w_in:
        copy.wait_recv()
    for cc in range(2):
        sq[cc] = jnp.zeros((8, 512), jnp.float32)
        for xh in range(2):

            @pl.loop(0, 7)
            def _(i):
                part = pl.ds(pl.multiple_of(i * 128, 128), 128)
                rows = pl.ds(pl.multiple_of((xh * 2 + core) * 896 + i * 128, 128), 128)
                merged = W[cc, xh, part].astype(jnp.float32) + jnp.dot(
                    left[rows], R[cc], preferred_element_type=jnp.float32
                )
                sq[cc] += jnp.sum((merged * merged).reshape(16, 8, 512), axis=0)
                W[cc, xh, part] = merged.astype(jnp.bfloat16)

    q_in = go(send(sq.at[1 - core], q_m, qs.at[7], qr.at[7], mate))
    q_in.wait_recv()
    q_t[...] = sq[core] + q_m[...]
    row_in = []
    for i, (dz, dx) in enumerate(rows_peers):
        row_in.append(go(send(q_t, q_r.at[i], qs.at[i], qr.at[i], at(dz=dz, dx=dx))))

    h_in.wait_recv()
    for s in range(2):
        block = H.at[y, 1 - xhi]
        y_in[s][1] = go(send(block, block, ys.at[s, 1], yr.at[s, 1], at(dy=1 if s == 0 else 3)))

    def pass_on(i):
        xh = xhi if i == 0 else 1 - xhi
        for s in range(2):
            y_in[s][i].wait_recv()
            part = H.at[(y + (3 if s == 0 else 1)) % 4, xh, pl.ds(4 * s, 4)]
            send(part, part, fs.at[s, i], fr.at[s, i], at(dy=1 if s == 0 else 3)).start()

    pass_on(0)
    keep.wait()
    for copy in row_in:
        copy.wait_recv()
    squares = q_t[...]
    for i in range(7):
        squares = squares + q_r[i]
    scale = column_scale(mag[...], jnp.sum(squares, axis=0, keepdims=True))

    def up_z(h):
        return at(dz=1 if h == 0 else 3)

    def down_z(h):
        return at(dz=3 if h == 0 else 1)

    def to_mate(i):
        return send(M_s.at[i], M_r.at[i], ms.at[i], mr.at[i], mate)

    def chain(i, h):
        return send(A_s.at[i, h], A_r.at[i, h], as_.at[i, h], ar.at[i, h], up_z(h))

    def direct(i, h):
        return send(B_s.at[i, h], B_r.at[i, h], bs.at[i, h], br.at[i, h], down_z(h))

    def last(i, h):
        return send(C_s.at[i, h], C_r.at[i, h], cs.at[i, h], cr.at[i, h], up_z(h))

    def aside(i):
        return send(D_s.at[i], D_r.at[i], ds.at[i], dr.at[i], at(dx=1))

    def block(i):
        b = (y + 3 * i + 3 * (i // 2) + 2 * (i // 3)) % 4

        def product(cc, n):
            cols = pl.ds(pl.multiple_of(n * 256, 256), 256)
            total = jnp.dot(
                H[b, 0].reshape(512, 896), W[cc, 0, :, cols], preferred_element_type=jnp.float32
            )
            return total + jnp.dot(
                H[b, 1].reshape(512, 896), W[cc, 1, :, cols], preferred_element_type=jnp.float32
            )

        @pl.loop(0, 2)
        def _(n):
            cols = pl.ds(pl.multiple_of(n * 256, 256), 256)
            M_s[i, :, cols] = product(1 - core, n).astype(jnp.bfloat16)

        to_mate(i).start()

        @pl.loop(0, 2)
        def _(n):
            cols = pl.ds(pl.multiple_of(n * 256, 256), 256)
            F[:, :, cols] = product(core, n).reshape(8, 64, 256)

        to_mate(i).wait_recv()
        F[...] += M_r[i].astype(jnp.float32).reshape(8, 64, 512)
        for h in range(2):
            A_s[i, h] = F[((z + 2) % 4) * 2 + h].astype(jnp.bfloat16)
            chain(i, h).start()
        for h in range(2):
            B_s[i, h] = F[((z + (3 if h == 0 else 1)) % 4) * 2 + h].astype(jnp.bfloat16)
            direct(i, h).start()
        for h in range(2):
            chain(i, h).wait_recv()
            value = F[((z + (1 if h == 0 else 3)) % 4) * 2 + h] + A_r[i, h].astype(jnp.float32)
            C_s[i, h] = value.astype(jnp.bfloat16)
            last(i, h).start()
        for h in range(2):
            direct(i, h).wait_recv()
            last(i, h).wait_recv()
            G[h] = F[z * 2 + h] + B_r[i, h].astype(jnp.float32) + C_r[i, h].astype(jnp.float32)
        D_s[i] = G[1 - xlo].astype(jnp.bfloat16)
        aside(i).start()
        aside(i).wait_recv()
        total = (G[xlo] + D_r[i].astype(jnp.float32)) * scale
        out[pl.ds(pl.multiple_of(b * 64, 64), 64), :] = total.astype(jnp.bfloat16)

    @pl.loop(0, 4)
    def _(i):
        @pl.when(i == 1)
        def _():
            pass_on(1)

        @pl.when(i == 3)
        def _():
            for s in range(2):
                for k in range(2):
                    part = H.at[(y + 2) % 4, (xhi, 1 - xhi)[k], pl.ds(4 * s, 4)]
                    send(part, part, fs.at[s, k], fr.at[s, k], at(dy=1 if s == 0 else 3)).wait_recv()

        block(i)

    for copy in started:
        copy.wait_send()
    for s in range(2):
        for k in range(2):
            part = H.at[(y + (3 if s == 0 else 1)) % 4, (xhi, 1 - xhi)[k], pl.ds(4 * s, 4)]
            send(part, part, fs.at[s, k], fr.at[s, k], at(dy=1 if s == 0 else 3)).wait_send()

    @pl.loop(0, 4)
    def _(i):
        to_mate(i).wait_send()
        aside(i).wait_send()
        for h in range(2):
            chain(i, h).wait_send()
            direct(i, h).wait_send()
            last(i, h).wait_send()


def mixed_of(hid, down_w, left, right, mag):
    anywhere = pl.BlockSpec(memory_space=pl.ANY)
    vmem = pl.BlockSpec(memory_space=pltpu.VMEM)
    dma = lambda *s: pltpu.SemaphoreType.DMA(s)
    bf = lambda *s: pltpu.VMEM(s, jnp.bfloat16)
    f32 = lambda *s: pltpu.VMEM(s, jnp.float32)
    piece = lambda: bf(4, 2, 64, 512)
    return pl.pallas_call(
        mix_kernel,
        out_shape=jax.ShapeDtypeStruct((256, 512), jnp.bfloat16),
        in_specs=[vmem, anywhere, vmem, vmem, vmem],
        out_specs=vmem,
        scratch_shapes=[
            bf(4, 2, 8, 64, 896), bf(2, 2, 896, 512), bf(2, 64, 512), bf(4, 512, 512), bf(4, 512, 512),
            f32(8, 64, 512), f32(2, 64, 512),
            piece(), piece(), piece(), piece(), piece(), piece(), bf(4, 64, 512), bf(4, 64, 512),
            f32(2, 8, 512), f32(8, 512), f32(8, 512), f32(7, 8, 512),
            dma(4), dma(1), dma(1), dma(2, 2), dma(2, 2), dma(2, 2), dma(2, 2), dma(3), dma(3),
            dma(4), dma(4), dma(4, 2), dma(4, 2), dma(4, 2), dma(4, 2), dma(4, 2), dma(4, 2),
            dma(4), dma(4), dma(8), dma(8),
        ],
        compiler_params=pltpu.CompilerParams(
            collective_id=1, has_side_effects=True, vmem_limit_bytes=60 * 2**20
        ),
        name="mix_kernel",
    )(hid, down_w, left, right, mag)


def shards(
    tokens,
    gate_frozen_weight, gate_left_factor, gate_right_factor, gate_column_magnitude,
    up_frozen_weight, up_left_factor, up_right_factor, up_column_magnitude,
    down_frozen_weight, down_left_factor, down_right_factor, down_column_magnitude,
):
    left = jnp.concatenate([gate_left_factor, up_left_factor], axis=1)
    hidden = hidden_of(
        tokens, gate_frozen_weight, up_frozen_weight, left, gate_right_factor, up_right_factor,
        gate_column_magnitude[None], up_column_magnitude[None],
    )
    return mixed_of(
        hidden, down_frozen_weight, down_left_factor, down_right_factor, down_column_magnitude[None]
    )


def solution(mesh):
    placed = (
        P("row", "col"),
        P("col", "row"), P("col", None), P(None, "row"), P("row"),
        P("col", "row"), P("col", None), P(None, "row"), P("row"),
        P("row", "col"), P("row", None), P(None, "col"), P("col"),
    )
    return jax.shard_map(
        shards, mesh=mesh, in_specs=placed, out_specs=P("row", "col"), check_vma=False
    )
```

```python
import functools

import jax
import jax.numpy as jnp
from jax import lax
from jax.experimental import pallas as pl
from jax.experimental.pallas import tpu as pltpu
from jax.sharding import PartitionSpec as P

stability_offset = 1e-06
MESH = pl.DeviceIdType.MESH
NJ = 7


def place():
    r = lax.axis_index("row")
    c = lax.axis_index("col")
    return r // 2, r % 2, c // 4, (c // 2) % 2, c % 2


def device(z, xlo, y, xhi, core):
    return (z * 2 + xlo, (y * 2 + xhi) * 2 + core)


def greet(peers):
    barrier = pltpu.get_barrier_semaphore()
    for peer in peers:
        pl.semaphore_signal(barrier, inc=1, device_id=peer, device_id_type=MESH)
    pl.semaphore_wait(barrier, len(peers))


def send(src, dst, ss, rs, peer):
    return pltpu.make_async_remote_copy(
        src_ref=src, dst_ref=dst, send_sem=ss, recv_sem=rs, device_id=peer, device_id_type=MESH
    )


def column_scale(magnitude, squares):
    return magnitude / jnp.sqrt(squares + stability_offset)


def hidden_kernel(
    tok, gate_w, up_w, left, gate_r, up_r, gate_m, up_m, hid,
    X, W, L, A_s, B_s, C_s, A_r, B_r, C_r, q_s, q_r,
    own, xs, xr, zs, zr, fs, fr, ds, dr, wl, ws, wr, ls, lr, as_, ar, bs, br, cs, cr, qs, qr,
):
    z, xlo, y, xhi, core = place()
    x = xhi * 2 + xlo
    q = xhi * 2 + core
    rb = z * 2 + xlo

    def at_x(d):
        n = (x + d) % 4
        return device(z, n % 2, y, n // 2, core)

    def at_z(d):
        return device((z + d) % 4, xlo, y, xhi, core)

    def at_y(d):
        return device(z, xlo, (y + d) % 4, xhi, core)

    mate = device(z, xlo, y, xhi, 1 - core)
    group = (mate, device(z, xlo, y, 1 - xhi, core), device(z, xlo, y, 1 - xhi, 1 - core))
    group_q = (xhi * 2 + 1 - core, (1 - xhi) * 2 + core, (1 - xhi) * 2 + 1 - core)
    greet((
        at_x(1), at_x(2), at_x(3), at_z(1), at_z(3), mate, group[2], at_y(1), at_y(2), at_y(3),
    ))

    def tile(dz, d, lo=0, n=256):
        xt = (x + 4 - d) % 4
        zt = (z + dz) % 4
        lane = pl.multiple_of(((xt // 2) * 2 + core) * 512, 512)
        return X.at[zt * 2 + xt % 2, pl.ds(lo, n), pl.ds(lane, 512)]

    mine = tile(0, 0)
    started = []

    def go(copy):
        copy.start()
        started.append(copy)
        return copy

    x_in = [None] * 4
    for d in (1, 3, 2):
        x_in[d] = go(send(tok, mine, xs.at[d - 1], xr.at[d - 1], at_x(d)))
    z_in = [[None] * 4, [None] * 4]
    z_in[0][0] = go(send(tok, mine, zs.at[0, 0], zr.at[0, 0], at_z(1)))
    z_in[1][0] = go(send(tok, mine, zs.at[1, 0], zr.at[1, 0], at_z(3)))
    d_in = [[None] * 4 for _ in range(4)]
    d_in[0][0] = go(send(tok, mine, ds.at[0, 0], dr.at[0, 0], mate))
    keep = pltpu.make_async_copy(tok, mine, own.at[0])
    keep.start()

    rows = pl.ds(pl.multiple_of(q * 512, 512), 512)
    l_in = [go(send(left, L.at[rows], ls.at[t], lr.at[t], group[t])) for t in range(3)]
    keep_l = pltpu.make_async_copy(left, L.at[rows], own.at[1])
    keep_l.start()

    def weight_copies(j):
        local, remote = [], []
        for g, w in enumerate((gate_w, up_w)):
            dst = W.at[j, rows, pl.ds(g * 128, 128)]
            for t in (1, 2, 0):
                cols = pl.ds(pl.multiple_of(group_q[t] * 896 + j * 128, 128), 128)
                remote.append(send(w.at[:, cols], dst, ws.at[j, g, t], wr.at[j, g, t], group[t]))
            cols = pl.ds(pl.multiple_of(q * 896 + j * 128, 128), 128)
            local.append(pltpu.make_async_copy(w.at[:, cols], dst, wl.at[j, g]))
        return local, remote

    def fetch(j):
        local, remote = weight_copies(j)
        for copy in remote + local:
            copy.start()


    for d in (1, 3, 2):
        x_in[d].wait_recv()
        here = tile(0, d)
        z_in[0][d] = go(send(here, here, zs.at[0, d], zr.at[0, d], at_z(1)))
        z_in[1][d] = go(send(here, here, zs.at[1, d], zr.at[1, d], at_z(3)))
        d_in[0][d] = go(send(here, here, ds.at[0, d], dr.at[0, d], mate))
    f_in = [[None] * 4, [None] * 4]
    for d in (0, 1, 3, 2):
        for s in range(2):
            z_in[s][d].wait_recv()
            dz = 3 if s == 0 else 1
            part = tile(dz, d, 128 * s, 128)
            f_in[s][d] = go(send(part, part, fs.at[s, d], fr.at[s, d], at_z(1 if s == 0 else 3)))
            here = tile(dz, d)
            d_in[1 + s][d] = go(send(here, here, ds.at[1 + s, d], dr.at[1 + s, d], mate))
    for d in (0, 1, 3, 2):
        f_in[0][d].wait_recv()
        f_in[1][d].wait_recv()
        here = tile(2, d)
        d_in[3][d] = go(send(here, here, ds.at[3, d], dr.at[3, d], mate))
    keep.wait()
    keep_l.wait()

    @pl.loop(0, NJ)
    def _(j):
        fetch(j)

    for copy in l_in:
        copy.wait_recv()
    for i in range(4):
        for d in range(4):
            d_in[i][d].wait_recv()

    def partial(b, h, j):
        t = X[pl.ds(4 * h, 4), pl.ds(pl.multiple_of(b * 64, 64), 64), :].reshape(256, 2048)
        return jnp.dot(t, W[j], preferred_element_type=jnp.float32)

    def chain(j, h):
        return send(A_s.at[j, h], A_r.at[j, h], as_.at[j, h], ar.at[j, h], at_y(1 if h == 0 else 3))

    def direct(j, h):
        return send(B_s.at[j, h], B_r.at[j, h], bs.at[j, h], br.at[j, h], at_y(3 if h == 0 else 1))

    def last(j, h):
        return send(C_s.at[j, h], C_r.at[j, h], cs.at[j, h], cr.at[j, h], at_y(1 if h == 0 else 3))

    def squares(j):
        return [send(q_s.at[j], q_r.at[j, d - 1], qs.at[j, d - 1], qr.at[j, d - 1], at_y(d)) for d in (1, 2, 3)]

    def finish(j):
        for copy in squares(j):
            copy.wait_recv()
        sq = jnp.sum(q_s[j] + q_r[j, 0] + q_r[j, 1] + q_r[j, 2], axis=0, keepdims=True)
        cols = pl.ds(pl.multiple_of(q * 896 + j * 128, 128), 128)
        gate_scale = column_scale(gate_m[:, cols], sq[:, :128])
        up_scale = column_scale(up_m[:, cols], sq[:, 128:])
        for h in range(2):
            direct(j, h).wait_recv()
            last(j, h).wait_recv()
            total = partial(y, h, j) + B_r[j, h].astype(jnp.float32) + C_r[j, h].astype(jnp.float32)
            gate = total[:, :128] * gate_scale
            up = total[:, 128:] * up_scale
            value = gate / (1.0 + jnp.exp(-gate)) * up
            hid[pl.ds(4 * h, 4), :, pl.ds(pl.multiple_of(j * 128, 128), 128)] = value.astype(
                jnp.bfloat16
            ).reshape(4, 64, 128)

    @pl.loop(0, NJ)
    def _(j):
        local, remote = weight_copies(j)
        for copy in local:
            copy.wait()
        for copy in remote:
            copy.wait_recv()
        cols = pl.ds(pl.multiple_of(q * 896 + j * 128, 128), 128)
        zero = jnp.zeros((64, 128), jnp.bfloat16)
        right = jnp.concatenate(
            [
                jnp.concatenate([gate_r[:, cols], zero], axis=1),
                jnp.concatenate([zero, up_r[:, cols]], axis=1),
            ],
            axis=0,
        )
        q_s[j] = jnp.zeros((8, 256), jnp.float32)

        @pl.loop(0, 8)
        def _(i):
            part = pl.ds(pl.multiple_of(i * 256, 256), 256)
            merged = W[j, part].astype(jnp.float32) + jnp.dot(
                L[part], right, preferred_element_type=jnp.float32
            )
            q_s[j] += jnp.sum((merged * merged).reshape(32, 8, 256), axis=0)
            W[j, part] = merged.astype(jnp.bfloat16)

        for h in range(2):
            A_s[j, h] = partial((y + 2) % 4, h, j).astype(jnp.bfloat16)
            chain(j, h).start()
        for copy in squares(j):
            copy.start()
        for h in range(2):
            B_s[j, h] = partial((y + (3 if h == 0 else 1)) % 4, h, j).astype(jnp.bfloat16)
            direct(j, h).start()
        for h in range(2):
            value = partial((y + (1 if h == 0 else 3)) % 4, h, j)
            chain(j, h).wait_recv()
            C_s[j, h] = (value + A_r[j, h].astype(jnp.float32)).astype(jnp.bfloat16)
            last(j, h).start()

        @pl.when(j >= 1)
        def _():
            finish(j - 1)

    finish(NJ - 1)

    for copy in started:
        copy.wait_send()

    @pl.loop(0, NJ)
    def _(j):
        for copy in weight_copies(j)[1] + squares(j):
            copy.wait_send()
        for h in range(2):
            chain(j, h).wait_send()
            direct(j, h).wait_send()
            last(j, h).wait_send()


def hidden_of(tok, gate_w, up_w, left, gate_r, up_r, gate_m, up_m):
    anywhere = pl.BlockSpec(memory_space=pl.ANY)
    vmem = pl.BlockSpec(memory_space=pltpu.VMEM)
    dma = lambda *s: pltpu.SemaphoreType.DMA(s)
    piece = lambda: pltpu.VMEM((NJ, 2, 256, 256), jnp.bfloat16)
    return pl.pallas_call(
        hidden_kernel,
        out_shape=jax.ShapeDtypeStruct((8, 64, 896), jnp.bfloat16),
        in_specs=[anywhere, anywhere, anywhere, vmem, vmem, vmem, vmem, vmem],
        out_specs=vmem,
        scratch_shapes=[
            pltpu.VMEM((8, 256, 2048), jnp.bfloat16),
            pltpu.VMEM((NJ, 2048, 256), jnp.bfloat16),
            pltpu.VMEM((2048, 128), jnp.bfloat16),
            piece(), piece(), piece(), piece(), piece(), piece(),
            pltpu.VMEM((NJ, 8, 256), jnp.float32),
            pltpu.VMEM((NJ, 3, 8, 256), jnp.float32),
            dma(2), dma(3), dma(3), dma(2, 4), dma(2, 4), dma(2, 4), dma(2, 4), dma(4, 4), dma(4, 4),
            dma(NJ, 2), dma(NJ, 2, 3), dma(NJ, 2, 3), dma(3), dma(3),
            dma(NJ, 2), dma(NJ, 2), dma(NJ, 2), dma(NJ, 2), dma(NJ, 2), dma(NJ, 2),
            dma(NJ, 3), dma(NJ, 3),
        ],
        compiler_params=pltpu.CompilerParams(
            collective_id=0, has_side_effects=True, vmem_limit_bytes=60 * 2**20
        ),
        name="hidden_kernel",
    )(tok, gate_w, up_w, left, gate_r, up_r, gate_m, up_m)


def mix_kernel(
    hid, down_w, left, right, mag, out,
    H, W, R, M_s, M_r, F, G, A_s, B_s, C_s, A_r, B_r, C_r, D_s, D_r, sq, q_m, q_t, q_r,
    own, hs, hr, ys, yr, fs, fr, ws, wr, ms, mr, as_, ar, bs, br, cs, cr, ds, dr, qs, qr,
):
    z, xlo, y, xhi, core = place()

    def at(dz=0, dx=0, dy=0):
        return device((z + dz) % 4, (xlo + dx) % 2, (y + dy) % 4, xhi, core)

    mate = device(z, xlo, y, xhi, 1 - core)
    across = device(z, xlo, y, 1 - xhi, core)
    rows_peers = [(dz, dx) for dz in range(4) for dx in range(2)][1:]
    greet([mate, across, at(dy=1), at(dy=3)] + [at(dz=dz, dx=dx) for dz, dx in rows_peers])
    started = []

    def go(copy):
        copy.start()
        started.append(copy)
        return copy

    h_in = go(send(hid, H.at[y, xhi], hs.at[0], hr.at[0], across))
    y_in = [[None, None], [None, None]]
    for s in range(2):
        y_in[s][0] = go(send(hid, H.at[y, xhi], ys.at[s, 0], yr.at[s, 0], at(dy=1 if s == 0 else 3)))
    keep = pltpu.make_async_copy(hid, H.at[y, xhi], own.at[0])
    keep.start()

    w_in, w_own = [], []
    w_in.append(go(send(right, R.at[core], ws.at[2], wr.at[2], mate)))
    for xh in range(2):
        theirs = pl.ds(pl.multiple_of((xh * 2 + 1 - core) * 896, 128), 896)
        ours = pl.ds(pl.multiple_of((xh * 2 + core) * 896, 128), 896)
        w_in.append(go(send(down_w.at[theirs], W.at[core, xh], ws.at[xh], wr.at[xh], mate)))
        w_own.append(pltpu.make_async_copy(down_w.at[ours], W.at[core, xh], own.at[1 + xh]))
    w_own.append(pltpu.make_async_copy(right, R.at[core], own.at[3]))
    for copy in w_own:
        copy.start()
    for copy in w_own:
        copy.wait()
    for copy in w_in:
        copy.wait_recv()
    for cc in range(2):
        sq[cc] = jnp.zeros((8, 512), jnp.float32)
        for xh in range(2):

            @pl.loop(0, 7)
            def _(i):
                part = pl.ds(pl.multiple_of(i * 128, 128), 128)
                rows = pl.ds(pl.multiple_of((xh * 2 + core) * 896 + i * 128, 128), 128)
                merged = W[cc, xh, part].astype(jnp.float32) + jnp.dot(
                    left[rows], R[cc], preferred_element_type=jnp.float32
                )
                sq[cc] += jnp.sum((merged * merged).reshape(16, 8, 512), axis=0)
                W[cc, xh, part] = merged.astype(jnp.bfloat16)

    q_in = go(send(sq.at[1 - core], q_m, qs.at[7], qr.at[7], mate))
    q_in.wait_recv()
    q_t[...] = sq[core] + q_m[...]
    row_in = []
    for i, (dz, dx) in enumerate(rows_peers):
        row_in.append(go(send(q_t, q_r.at[i], qs.at[i], qr.at[i], at(dz=dz, dx=dx))))

    h_in.wait_recv()
    for s in range(2):
        block = H.at[y, 1 - xhi]
        y_in[s][1] = go(send(block, block, ys.at[s, 1], yr.at[s, 1], at(dy=1 if s == 0 else 3)))

    def pass_on(i):
        xh = xhi if i == 0 else 1 - xhi
        for s in range(2):
            y_in[s][i].wait_recv()
            part = H.at[(y + (3 if s == 0 else 1)) % 4, xh, pl.ds(4 * s, 4)]
            send(part, part, fs.at[s, i], fr.at[s, i], at(dy=1 if s == 0 else 3)).start()

    pass_on(0)
    keep.wait()
    for copy in row_in:
        copy.wait_recv()
    squares = q_t[...]
    for i in range(7):
        squares = squares + q_r[i]
    scale = column_scale(mag[...], jnp.sum(squares, axis=0, keepdims=True))

    def up_z(h):
        return at(dz=1 if h == 0 else 3)

    def down_z(h):
        return at(dz=3 if h == 0 else 1)

    def to_mate(i):
        return send(M_s.at[i], M_r.at[i], ms.at[i], mr.at[i], mate)

    def chain(i, h):
        return send(A_s.at[i, h], A_r.at[i, h], as_.at[i, h], ar.at[i, h], up_z(h))

    def direct(i, h):
        return send(B_s.at[i, h], B_r.at[i, h], bs.at[i, h], br.at[i, h], down_z(h))

    def last(i, h):
        return send(C_s.at[i, h], C_r.at[i, h], cs.at[i, h], cr.at[i, h], up_z(h))

    def aside(i):
        return send(D_s.at[i], D_r.at[i], ds.at[i], dr.at[i], at(dx=1))

    def block(i):
        b = (y + 3 * i + 3 * (i // 2) + 2 * (i // 3)) % 4

        def product(cc, n):
            cols = pl.ds(pl.multiple_of(n * 256, 256), 256)
            total = jnp.dot(
                H[b, 0].reshape(512, 896), W[cc, 0, :, cols], preferred_element_type=jnp.float32
            )
            return total + jnp.dot(
                H[b, 1].reshape(512, 896), W[cc, 1, :, cols], preferred_element_type=jnp.float32
            )

        @pl.loop(0, 2)
        def _(n):
            cols = pl.ds(pl.multiple_of(n * 256, 256), 256)
            M_s[i, :, cols] = product(1 - core, n).astype(jnp.bfloat16)

        to_mate(i).start()

        @pl.loop(0, 2)
        def _(n):
            cols = pl.ds(pl.multiple_of(n * 256, 256), 256)
            F[:, :, cols] = product(core, n).reshape(8, 64, 256)

        to_mate(i).wait_recv()
        F[...] += M_r[i].astype(jnp.float32).reshape(8, 64, 512)
        for h in range(2):
            A_s[i, h] = F[((z + 2) % 4) * 2 + h].astype(jnp.bfloat16)
            chain(i, h).start()
        for h in range(2):
            B_s[i, h] = F[((z + (3 if h == 0 else 1)) % 4) * 2 + h].astype(jnp.bfloat16)
            direct(i, h).start()
        for h in range(2):
            chain(i, h).wait_recv()
            value = F[((z + (1 if h == 0 else 3)) % 4) * 2 + h] + A_r[i, h].astype(jnp.float32)
            C_s[i, h] = value.astype(jnp.bfloat16)
            last(i, h).start()
        for h in range(2):
            direct(i, h).wait_recv()
            last(i, h).wait_recv()
            G[h] = F[z * 2 + h] + B_r[i, h].astype(jnp.float32) + C_r[i, h].astype(jnp.float32)
        D_s[i] = G[1 - xlo].astype(jnp.bfloat16)
        aside(i).start()
        aside(i).wait_recv()
        total = (G[xlo] + D_r[i].astype(jnp.float32)) * scale
        out[pl.ds(pl.multiple_of(b * 64, 64), 64), :] = total.astype(jnp.bfloat16)

    @pl.loop(0, 4)
    def _(i):
        @pl.when(i == 1)
        def _():
            pass_on(1)

        @pl.when(i == 3)
        def _():
            for s in range(2):
                for k in range(2):
                    part = H.at[(y + 2) % 4, (xhi, 1 - xhi)[k], pl.ds(4 * s, 4)]
                    send(part, part, fs.at[s, k], fr.at[s, k], at(dy=1 if s == 0 else 3)).wait_recv()

        block(i)

    for copy in started:
        copy.wait_send()
    for s in range(2):
        for k in range(2):
            part = H.at[(y + (3 if s == 0 else 1)) % 4, (xhi, 1 - xhi)[k], pl.ds(4 * s, 4)]
            send(part, part, fs.at[s, k], fr.at[s, k], at(dy=1 if s == 0 else 3)).wait_send()

    @pl.loop(0, 4)
    def _(i):
        to_mate(i).wait_send()
        aside(i).wait_send()
        for h in range(2):
            chain(i, h).wait_send()
            direct(i, h).wait_send()
            last(i, h).wait_send()


def mixed_of(hid, down_w, left, right, mag):
    anywhere = pl.BlockSpec(memory_space=pl.ANY)
    vmem = pl.BlockSpec(memory_space=pltpu.VMEM)
    dma = lambda *s: pltpu.SemaphoreType.DMA(s)
    bf = lambda *s: pltpu.VMEM(s, jnp.bfloat16)
    f32 = lambda *s: pltpu.VMEM(s, jnp.float32)
    piece = lambda: bf(4, 2, 64, 512)
    return pl.pallas_call(
        mix_kernel,
        out_shape=jax.ShapeDtypeStruct((256, 512), jnp.bfloat16),
        in_specs=[vmem, anywhere, vmem, vmem, vmem],
        out_specs=vmem,
        scratch_shapes=[
            bf(4, 2, 8, 64, 896), bf(2, 2, 896, 512), bf(2, 64, 512), bf(4, 512, 512), bf(4, 512, 512),
            f32(8, 64, 512), f32(2, 64, 512),
            piece(), piece(), piece(), piece(), piece(), piece(), bf(4, 64, 512), bf(4, 64, 512),
            f32(2, 8, 512), f32(8, 512), f32(8, 512), f32(7, 8, 512),
            dma(4), dma(1), dma(1), dma(2, 2), dma(2, 2), dma(2, 2), dma(2, 2), dma(3), dma(3),
            dma(4), dma(4), dma(4, 2), dma(4, 2), dma(4, 2), dma(4, 2), dma(4, 2), dma(4, 2),
            dma(4), dma(4), dma(8), dma(8),
        ],
        compiler_params=pltpu.CompilerParams(
            collective_id=1, has_side_effects=True, vmem_limit_bytes=60 * 2**20
        ),
        name="mix_kernel",
    )(hid, down_w, left, right, mag)


def shards(
    tokens,
    gate_frozen_weight, gate_left_factor, gate_right_factor, gate_column_magnitude,
    up_frozen_weight, up_left_factor, up_right_factor, up_column_magnitude,
    down_frozen_weight, down_left_factor, down_right_factor, down_column_magnitude,
):
    left = jnp.concatenate([gate_left_factor, up_left_factor], axis=1)
    hidden = hidden_of(
        tokens, gate_frozen_weight, up_frozen_weight, left, gate_right_factor, up_right_factor,
        gate_column_magnitude[None], up_column_magnitude[None],
    )
    return mixed_of(
        hidden, down_frozen_weight, down_left_factor, down_right_factor, down_column_magnitude[None]
    )


def solution(mesh):
    placed = (
        P("row", "col"),
        P("col", "row"), P("col", None), P(None, "row"), P("row"),
        P("col", "row"), P("col", None), P(None, "row"), P("row"),
        P("row", "col"), P("row", None), P(None, "col"), P("col"),
    )
    return jax.shard_map(
        shards, mesh=mesh, in_specs=placed, out_specs=P("row", "col"), check_vma=False
    )
```

```python
import functools

import jax
import jax.numpy as jnp
from jax import lax
from jax.experimental import pallas as pl
from jax.experimental.pallas import tpu as pltpu
from jax.sharding import PartitionSpec as P

stability_offset = 1e-06
MESH = pl.DeviceIdType.MESH
NJ = 7


def place():
    r = lax.axis_index("row")
    c = lax.axis_index("col")
    return r // 2, r % 2, c // 4, (c // 2) % 2, c % 2


def device(z, xlo, y, xhi, core):
    return (z * 2 + xlo, (y * 2 + xhi) * 2 + core)


def greet(peers):
    barrier = pltpu.get_barrier_semaphore()
    for peer in peers:
        pl.semaphore_signal(barrier, inc=1, device_id=peer, device_id_type=MESH)
    pl.semaphore_wait(barrier, len(peers))


def send(src, dst, ss, rs, peer):
    return pltpu.make_async_remote_copy(
        src_ref=src, dst_ref=dst, send_sem=ss, recv_sem=rs, device_id=peer, device_id_type=MESH
    )


def column_scale(magnitude, squares):
    return magnitude / jnp.sqrt(squares + stability_offset)


def hidden_kernel(
    tok, gate_w, up_w, left, gate_r, up_r, gate_m, up_m, hid,
    X, W, L, A_s, B_s, C_s, A_r, B_r, C_r, q_s, q_r,
    own, xs, xr, zs, zr, fs, fr, ds, dr, wl, ws, wr, ls, lr, as_, ar, bs, br, cs, cr, qs, qr,
):
    z, xlo, y, xhi, core = place()
    x = xhi * 2 + xlo
    q = xhi * 2 + core
    rb = z * 2 + xlo

    def at_x(d):
        n = (x + d) % 4
        return device(z, n % 2, y, n // 2, core)

    def at_z(d):
        return device((z + d) % 4, xlo, y, xhi, core)

    def at_y(d):
        return device(z, xlo, (y + d) % 4, xhi, core)

    mate = device(z, xlo, y, xhi, 1 - core)
    group = (mate, device(z, xlo, y, 1 - xhi, core), device(z, xlo, y, 1 - xhi, 1 - core))
    group_q = (xhi * 2 + 1 - core, (1 - xhi) * 2 + core, (1 - xhi) * 2 + 1 - core)
    greet((
        at_x(1), at_x(2), at_x(3), at_z(1), at_z(3), mate, group[2], at_y(1), at_y(2), at_y(3),
    ))

    def tile(dz, d, lo=0, n=256):
        xt = (x + 4 - d) % 4
        zt = (z + dz) % 4
        lane = pl.multiple_of(((xt // 2) * 2 + core) * 512, 512)
        return X.at[zt * 2 + xt % 2, pl.ds(lo, n), pl.ds(lane, 512)]

    mine = tile(0, 0)
    started = []

    def go(copy):
        copy.start()
        started.append(copy)
        return copy

    x_in = [None] * 4
    for d in (1, 3, 2):
        x_in[d] = go(send(tok, mine, xs.at[d - 1], xr.at[d - 1], at_x(d)))
    z_in = [[None] * 4, [None] * 4]
    z_in[0][0] = go(send(tok, mine, zs.at[0, 0], zr.at[0, 0], at_z(1)))
    z_in[1][0] = go(send(tok, mine, zs.at[1, 0], zr.at[1, 0], at_z(3)))
    d_in = [[None] * 4 for _ in range(4)]
    d_in[0][0] = go(send(tok, mine, ds.at[0, 0], dr.at[0, 0], mate))
    keep = pltpu.make_async_copy(tok, mine, own.at[0])
    keep.start()

    rows = pl.ds(pl.multiple_of(q * 512, 512), 512)
    l_in = [go(send(left, L.at[rows], ls.at[t], lr.at[t], group[t])) for t in range(3)]
    keep_l = pltpu.make_async_copy(left, L.at[rows], own.at[1])
    keep_l.start()

    def weight_copies(j):
        local, remote = [], []
        for g, w in enumerate((gate_w, up_w)):
            dst = W.at[j, rows, pl.ds(g * 128, 128)]
            for t in (1, 2, 0):
                cols = pl.ds(pl.multiple_of(group_q[t] * 896 + j * 128, 128), 128)
                remote.append(send(w.at[:, cols], dst, ws.at[j, g, t], wr.at[j, g, t], group[t]))
            cols = pl.ds(pl.multiple_of(q * 896 + j * 128, 128), 128)
            local.append(pltpu.make_async_copy(w.at[:, cols], dst, wl.at[j, g]))
        return local, remote

    def fetch(j):
        local, remote = weight_copies(j)
        for copy in remote + local:
            copy.start()


    for d in (1, 3, 2):
        x_in[d].wait_recv()
        here = tile(0, d)
        z_in[0][d] = go(send(here, here, zs.at[0, d], zr.at[0, d], at_z(1)))
        z_in[1][d] = go(send(here, here, zs.at[1, d], zr.at[1, d], at_z(3)))
        d_in[0][d] = go(send(here, here, ds.at[0, d], dr.at[0, d], mate))
    f_in = [[None] * 4, [None] * 4]
    for d in (0, 1, 3, 2):
        for s in range(2):
            z_in[s][d].wait_recv()
            dz = 3 if s == 0 else 1
            part = tile(dz, d, 128 * s, 128)
            f_in[s][d] = go(send(part, part, fs.at[s, d], fr.at[s, d], at_z(1 if s == 0 else 3)))
            here = tile(dz, d)
            d_in[1 + s][d] = go(send(here, here, ds.at[1 + s, d], dr.at[1 + s, d], mate))
        if d == 3:

            @pl.loop(0, NJ)
            def _(j):
                fetch(j)

    for d in (0, 1, 3, 2):
        f_in[0][d].wait_recv()
        f_in[1][d].wait_recv()
        here = tile(2, d)
        d_in[3][d] = go(send(here, here, ds.at[3, d], dr.at[3, d], mate))
    keep.wait()
    keep_l.wait()
    for copy in l_in:
        copy.wait_recv()
    for i in range(4):
        for d in range(4):
            d_in[i][d].wait_recv()

    def partial(b, h, j):
        t = X[pl.ds(4 * h, 4), pl.ds(pl.multiple_of(b * 64, 64), 64), :].reshape(256, 2048)
        return jnp.dot(t, W[j], preferred_element_type=jnp.float32)

    def chain(j, h):
        return send(A_s.at[j, h], A_r.at[j, h], as_.at[j, h], ar.at[j, h], at_y(1 if h == 0 else 3))

    def direct(j, h):
        return send(B_s.at[j, h], B_r.at[j, h], bs.at[j, h], br.at[j, h], at_y(3 if h == 0 else 1))

    def last(j, h):
        return send(C_s.at[j, h], C_r.at[j, h], cs.at[j, h], cr.at[j, h], at_y(1 if h == 0 else 3))

    def squares(j):
        return [send(q_s.at[j], q_r.at[j, d - 1], qs.at[j, d - 1], qr.at[j, d - 1], at_y(d)) for d in (1, 2, 3)]

    def finish(j):
        for copy in squares(j):
            copy.wait_recv()
        sq = jnp.sum(q_s[j] + q_r[j, 0] + q_r[j, 1] + q_r[j, 2], axis=0, keepdims=True)
        cols = pl.ds(pl.multiple_of(q * 896 + j * 128, 128), 128)
        gate_scale = column_scale(gate_m[cols][None], sq[:, :128])
        up_scale = column_scale(up_m[cols][None], sq[:, 128:])
        for h in range(2):
            direct(j, h).wait_recv()
            last(j, h).wait_recv()
            total = partial(y, h, j) + B_r[j, h].astype(jnp.float32) + C_r[j, h].astype(jnp.float32)
            gate = total[:, :128] * gate_scale
            up = total[:, 128:] * up_scale
            value = gate / (1.0 + jnp.exp(-gate)) * up
            hid[pl.ds(4 * h, 4), :, pl.ds(pl.multiple_of(j * 128, 128), 128)] = value.astype(
                jnp.bfloat16
            ).reshape(4, 64, 128)

    @pl.loop(0, NJ)
    def _(j):
        local, remote = weight_copies(j)
        for copy in local:
            copy.wait()
        for copy in remote:
            copy.wait_recv()
        cols = pl.ds(pl.multiple_of(q * 896 + j * 128, 128), 128)
        zero = jnp.zeros((64, 128), jnp.bfloat16)
        right = jnp.concatenate(
            [
                jnp.concatenate([gate_r[:, cols], zero], axis=1),
                jnp.concatenate([zero, up_r[:, cols]], axis=1),
            ],
            axis=0,
        )
        q_s[j] = jnp.zeros((8, 256), jnp.float32)

        @pl.loop(0, 8)
        def _(i):
            part = pl.ds(pl.multiple_of(i * 256, 256), 256)
            merged = W[j, part].astype(jnp.float32) + jnp.dot(
                L[part], right, preferred_element_type=jnp.float32
            )
            q_s[j] += jnp.sum((merged * merged).reshape(32, 8, 256), axis=0)
            W[j, part] = merged.astype(jnp.bfloat16)

        for h in range(2):
            A_s[j, h] = partial((y + 2) % 4, h, j).astype(jnp.bfloat16)
            chain(j, h).start()
        for copy in squares(j):
            copy.start()
        for h in range(2):
            B_s[j, h] = partial((y + (3 if h == 0 else 1)) % 4, h, j).astype(jnp.bfloat16)
            direct(j, h).start()
        for h in range(2):
            value = partial((y + (1 if h == 0 else 3)) % 4, h, j)
            chain(j, h).wait_recv()
            C_s[j, h] = (value + A_r[j, h].astype(jnp.float32)).astype(jnp.bfloat16)
            last(j, h).start()

        @pl.when(j >= 1)
        def _():
            finish(j - 1)

    finish(NJ - 1)

    for copy in started:
        copy.wait_send()

    @pl.loop(0, NJ)
    def _(j):
        for copy in weight_copies(j)[1] + squares(j):
            copy.wait_send()
        for h in range(2):
            chain(j, h).wait_send()
            direct(j, h).wait_send()
            last(j, h).wait_send()


def hidden_of(tok, gate_w, up_w, left, gate_r, up_r, gate_m, up_m):
    anywhere = pl.BlockSpec(memory_space=pl.ANY)
    vmem = pl.BlockSpec(memory_space=pltpu.VMEM)
    dma = lambda *s: pltpu.SemaphoreType.DMA(s)
    piece = lambda: pltpu.VMEM((NJ, 2, 256, 256), jnp.bfloat16)
    return pl.pallas_call(
        hidden_kernel,
        out_shape=jax.ShapeDtypeStruct((8, 64, 896), jnp.bfloat16),
        in_specs=[anywhere, anywhere, anywhere, vmem, vmem, vmem, vmem, vmem],
        out_specs=vmem,
        scratch_shapes=[
            pltpu.VMEM((8, 256, 2048), jnp.bfloat16),
            pltpu.VMEM((NJ, 2048, 256), jnp.bfloat16),
            pltpu.VMEM((2048, 128), jnp.bfloat16),
            piece(), piece(), piece(), piece(), piece(), piece(),
            pltpu.VMEM((NJ, 8, 256), jnp.float32),
            pltpu.VMEM((NJ, 3, 8, 256), jnp.float32),
            dma(2), dma(3), dma(3), dma(2, 4), dma(2, 4), dma(2, 4), dma(2, 4), dma(4, 4), dma(4, 4),
            dma(NJ, 2), dma(NJ, 2, 3), dma(NJ, 2, 3), dma(3), dma(3),
            dma(NJ, 2), dma(NJ, 2), dma(NJ, 2), dma(NJ, 2), dma(NJ, 2), dma(NJ, 2),
            dma(NJ, 3), dma(NJ, 3),
        ],
        compiler_params=pltpu.CompilerParams(
            collective_id=0, has_side_effects=True, vmem_limit_bytes=60 * 2**20
        ),
        name="hidden_kernel",
    )(tok, gate_w, up_w, left, gate_r, up_r, gate_m, up_m)


def mix_kernel(
    hid, down_w, left, right, mag, out,
    H, W, R, M_s, M_r, F, G, A_s, B_s, C_s, A_r, B_r, C_r, D_s, D_r, sq, q_m, q_t, q_r,
    own, hs, hr, ys, yr, fs, fr, ws, wr, ms, mr, as_, ar, bs, br, cs, cr, ds, dr, qs, qr,
):
    z, xlo, y, xhi, core = place()

    def at(dz=0, dx=0, dy=0):
        return device((z + dz) % 4, (xlo + dx) % 2, (y + dy) % 4, xhi, core)

    mate = device(z, xlo, y, xhi, 1 - core)
    across = device(z, xlo, y, 1 - xhi, core)
    rows_peers = [(dz, dx) for dz in range(4) for dx in range(2)][1:]
    greet([mate, across, at(dy=1), at(dy=3)] + [at(dz=dz, dx=dx) for dz, dx in rows_peers])
    started = []

    def go(copy):
        copy.start()
        started.append(copy)
        return copy

    h_in = go(send(hid, H.at[y, xhi], hs.at[0], hr.at[0], across))
    y_in = [[None, None], [None, None]]
    for s in range(2):
        y_in[s][0] = go(send(hid, H.at[y, xhi], ys.at[s, 0], yr.at[s, 0], at(dy=1 if s == 0 else 3)))
    keep = pltpu.make_async_copy(hid, H.at[y, xhi], own.at[0])
    keep.start()

    w_in, w_own = [], []
    w_in.append(go(send(right, R.at[core], ws.at[2], wr.at[2], mate)))
    for xh in range(2):
        theirs = pl.ds(pl.multiple_of((xh * 2 + 1 - core) * 896, 128), 896)
        ours = pl.ds(pl.multiple_of((xh * 2 + core) * 896, 128), 896)
        w_in.append(go(send(down_w.at[theirs], W.at[core, xh], ws.at[xh], wr.at[xh], mate)))
        w_own.append(pltpu.make_async_copy(down_w.at[ours], W.at[core, xh], own.at[1 + xh]))
    w_own.append(pltpu.make_async_copy(right, R.at[core], own.at[3]))
    for copy in w_own:
        copy.start()
    for copy in w_own:
        copy.wait()
    for copy in w_in:
        copy.wait_recv()
    for cc in range(2):
        sq[cc] = jnp.zeros((8, 512), jnp.float32)
        for xh in range(2):

            @pl.loop(0, 7)
            def _(i):
                part = pl.ds(pl.multiple_of(i * 128, 128), 128)
                rows = pl.ds(pl.multiple_of((xh * 2 + core) * 896 + i * 128, 128), 128)
                merged = W[cc, xh, part].astype(jnp.float32) + jnp.dot(
                    left[rows], R[cc], preferred_element_type=jnp.float32
                )
                sq[cc] += jnp.sum((merged * merged).reshape(16, 8, 512), axis=0)
                W[cc, xh, part] = merged.astype(jnp.bfloat16)

    q_in = go(send(sq.at[1 - core], q_m, qs.at[7], qr.at[7], mate))
    q_in.wait_recv()
    q_t[...] = sq[core] + q_m[...]
    row_in = []
    for i, (dz, dx) in enumerate(rows_peers):
        row_in.append(go(send(q_t, q_r.at[i], qs.at[i], qr.at[i], at(dz=dz, dx=dx))))

    h_in.wait_recv()
    for s in range(2):
        block = H.at[y, 1 - xhi]
        y_in[s][1] = go(send(block, block, ys.at[s, 1], yr.at[s, 1], at(dy=1 if s == 0 else 3)))

    def pass_on(i):
        xh = xhi if i == 0 else 1 - xhi
        for s in range(2):
            y_in[s][i].wait_recv()
            part = H.at[(y + (3 if s == 0 else 1)) % 4, xh, pl.ds(4 * s, 4)]
            send(part, part, fs.at[s, i], fr.at[s, i], at(dy=1 if s == 0 else 3)).start()

    pass_on(0)
    keep.wait()
    for copy in row_in:
        copy.wait_recv()
    squares = q_t[...]
    for i in range(7):
        squares = squares + q_r[i]
    scale = column_scale(mag[...][None], jnp.sum(squares, axis=0, keepdims=True))

    def up_z(h):
        return at(dz=1 if h == 0 else 3)

    def down_z(h):
        return at(dz=3 if h == 0 else 1)

    def to_mate(i):
        return send(M_s.at[i], M_r.at[i], ms.at[i], mr.at[i], mate)

    def chain(i, h):
        return send(A_s.at[i, h], A_r.at[i, h], as_.at[i, h], ar.at[i, h], up_z(h))

    def direct(i, h):
        return send(B_s.at[i, h], B_r.at[i, h], bs.at[i, h], br.at[i, h], down_z(h))

    def last(i, h):
        return send(C_s.at[i, h], C_r.at[i, h], cs.at[i, h], cr.at[i, h], up_z(h))

    def aside(i):
        return send(D_s.at[i], D_r.at[i], ds.at[i], dr.at[i], at(dx=1))

    def block(i):
        b = (y + 3 * i + 3 * (i // 2) + 2 * (i // 3)) % 4

        def product(cc, n):
            cols = pl.ds(pl.multiple_of(n * 256, 256), 256)
            total = jnp.dot(
                H[b, 0].reshape(512, 896), W[cc, 0, :, cols], preferred_element_type=jnp.float32
            )
            return total + jnp.dot(
                H[b, 1].reshape(512, 896), W[cc, 1, :, cols], preferred_element_type=jnp.float32
            )

        @pl.loop(0, 2)
        def _(n):
            cols = pl.ds(pl.multiple_of(n * 256, 256), 256)
            M_s[i, :, cols] = product(1 - core, n).astype(jnp.bfloat16)

        to_mate(i).start()

        @pl.loop(0, 2)
        def _(n):
            cols = pl.ds(pl.multiple_of(n * 256, 256), 256)
            F[:, :, cols] = product(core, n).reshape(8, 64, 256)

        to_mate(i).wait_recv()
        F[...] += M_r[i].astype(jnp.float32).reshape(8, 64, 512)
        for h in range(2):
            A_s[i, h] = F[((z + 2) % 4) * 2 + h].astype(jnp.bfloat16)
            chain(i, h).start()
        for h in range(2):
            B_s[i, h] = F[((z + (3 if h == 0 else 1)) % 4) * 2 + h].astype(jnp.bfloat16)
            direct(i, h).start()
        for h in range(2):
            chain(i, h).wait_recv()
            value = F[((z + (1 if h == 0 else 3)) % 4) * 2 + h] + A_r[i, h].astype(jnp.float32)
            C_s[i, h] = value.astype(jnp.bfloat16)
            last(i, h).start()
        for h in range(2):
            direct(i, h).wait_recv()
            last(i, h).wait_recv()
            G[h] = F[z * 2 + h] + B_r[i, h].astype(jnp.float32) + C_r[i, h].astype(jnp.float32)
        D_s[i] = G[1 - xlo].astype(jnp.bfloat16)
        aside(i).start()
        aside(i).wait_recv()
        total = (G[xlo] + D_r[i].astype(jnp.float32)) * scale
        out[pl.ds(pl.multiple_of(b * 64, 64), 64), :] = total.astype(jnp.bfloat16)

    @pl.loop(0, 4)
    def _(i):
        @pl.when(i == 1)
        def _():
            pass_on(1)

        @pl.when(i == 3)
        def _():
            for s in range(2):
                for k in range(2):
                    part = H.at[(y + 2) % 4, (xhi, 1 - xhi)[k], pl.ds(4 * s, 4)]
                    send(part, part, fs.at[s, k], fr.at[s, k], at(dy=1 if s == 0 else 3)).wait_recv()

        block(i)

    for copy in started:
        copy.wait_send()
    for s in range(2):
        for k in range(2):
            part = H.at[(y + (3 if s == 0 else 1)) % 4, (xhi, 1 - xhi)[k], pl.ds(4 * s, 4)]
            send(part, part, fs.at[s, k], fr.at[s, k], at(dy=1 if s == 0 else 3)).wait_send()

    @pl.loop(0, 4)
    def _(i):
        to_mate(i).wait_send()
        aside(i).wait_send()
        for h in range(2):
            chain(i, h).wait_send()
            direct(i, h).wait_send()
            last(i, h).wait_send()


def mixed_of(hid, down_w, left, right, mag):
    anywhere = pl.BlockSpec(memory_space=pl.ANY)
    vmem = pl.BlockSpec(memory_space=pltpu.VMEM)
    dma = lambda *s: pltpu.SemaphoreType.DMA(s)
    bf = lambda *s: pltpu.VMEM(s, jnp.bfloat16)
    f32 = lambda *s: pltpu.VMEM(s, jnp.float32)
    piece = lambda: bf(4, 2, 64, 512)
    return pl.pallas_call(
        mix_kernel,
        out_shape=jax.ShapeDtypeStruct((256, 512), jnp.bfloat16),
        in_specs=[vmem, anywhere, vmem, vmem, vmem],
        out_specs=vmem,
        scratch_shapes=[
            bf(4, 2, 8, 64, 896), bf(2, 2, 896, 512), bf(2, 64, 512), bf(4, 512, 512), bf(4, 512, 512),
            f32(8, 64, 512), f32(2, 64, 512),
            piece(), piece(), piece(), piece(), piece(), piece(), bf(4, 64, 512), bf(4, 64, 512),
            f32(2, 8, 512), f32(8, 512), f32(8, 512), f32(7, 8, 512),
            dma(4), dma(1), dma(1), dma(2, 2), dma(2, 2), dma(2, 2), dma(2, 2), dma(3), dma(3),
            dma(4), dma(4), dma(4, 2), dma(4, 2), dma(4, 2), dma(4, 2), dma(4, 2), dma(4, 2),
            dma(4), dma(4), dma(8), dma(8),
        ],
        compiler_params=pltpu.CompilerParams(
            collective_id=1, has_side_effects=True, vmem_limit_bytes=60 * 2**20
        ),
        name="mix_kernel",
    )(hid, down_w, left, right, mag)


def shards(
    tokens,
    gate_frozen_weight, gate_left_factor, gate_right_factor, gate_column_magnitude,
    up_frozen_weight, up_left_factor, up_right_factor, up_column_magnitude,
    down_frozen_weight, down_left_factor, down_right_factor, down_column_magnitude,
):
    left = jnp.concatenate([gate_left_factor, up_left_factor], axis=1)
    hidden = hidden_of(
        tokens, gate_frozen_weight, up_frozen_weight, left, gate_right_factor, up_right_factor,
        gate_column_magnitude, up_column_magnitude,
    )
    return mixed_of(
        hidden, down_frozen_weight, down_left_factor, down_right_factor, down_column_magnitude
    )


def solution(mesh):
    placed = (
        P("row", "col"),
        P("col", "row"), P("col", None), P(None, "row"), P("row"),
        P("col", "row"), P("col", None), P(None, "row"), P("row"),
        P("row", "col"), P("row", None), P(None, "col"), P("col"),
    )
    return jax.shard_map(
        shards, mesh=mesh, in_specs=placed, out_specs=P("row", "col"), check_vma=False
    )
```

```python
import functools

import jax
import jax.numpy as jnp
from jax import lax
from jax.experimental import pallas as pl
from jax.experimental.pallas import tpu as pltpu
from jax.sharding import PartitionSpec as P

stability_offset = 1e-06
MESH = pl.DeviceIdType.MESH
NJ = 7


def place():
    r = lax.axis_index("row")
    c = lax.axis_index("col")
    return r // 2, r % 2, c // 4, (c // 2) % 2, c % 2


def device(z, xlo, y, xhi, core):
    return (z * 2 + xlo, (y * 2 + xhi) * 2 + core)


def greet(peers):
    barrier = pltpu.get_barrier_semaphore()
    for peer in peers:
        pl.semaphore_signal(barrier, inc=1, device_id=peer, device_id_type=MESH)
    pl.semaphore_wait(barrier, len(peers))


def send(src, dst, ss, rs, peer):
    return pltpu.make_async_remote_copy(
        src_ref=src, dst_ref=dst, send_sem=ss, recv_sem=rs, device_id=peer, device_id_type=MESH
    )


def column_scale(magnitude, squares):
    return magnitude / jnp.sqrt(squares + stability_offset)


def hidden_kernel(
    tok, gate_w, up_w, left, gate_r, up_r, gate_m, up_m, hid,
    X, W, L, A_s, B_s, C_s, A_r, B_r, C_r, q_s, q_r,
    own, xs, xr, zs, zr, fs, fr, ds, dr, wl, ws, wr, ls, lr, as_, ar, bs, br, cs, cr, qs, qr,
):
    z, xlo, y, xhi, core = place()
    x = xhi * 2 + xlo
    q = xhi * 2 + core
    rb = z * 2 + xlo

    def at_x(d):
        n = (x + d) % 4
        return device(z, n % 2, y, n // 2, core)

    def at_z(d):
        return device((z + d) % 4, xlo, y, xhi, core)

    def at_y(d):
        return device(z, xlo, (y + d) % 4, xhi, core)

    mate = device(z, xlo, y, xhi, 1 - core)
    group = (mate, device(z, xlo, y, 1 - xhi, core), device(z, xlo, y, 1 - xhi, 1 - core))
    group_q = (xhi * 2 + 1 - core, (1 - xhi) * 2 + core, (1 - xhi) * 2 + 1 - core)
    greet((
        at_x(1), at_x(2), at_x(3), at_z(1), at_z(3), mate, group[2], at_y(1), at_y(2), at_y(3),
    ))

    def tile(dz, d, lo=0, n=256):
        xt = (x + 4 - d) % 4
        zt = (z + dz) % 4
        lane = pl.multiple_of(((xt // 2) * 2 + core) * 512, 512)
        return X.at[zt * 2 + xt % 2, pl.ds(lo, n), pl.ds(lane, 512)]

    mine = tile(0, 0)
    started = []

    def go(copy):
        copy.start()
        started.append(copy)
        return copy

    x_in = [None] * 4
    for d in (1, 3, 2):
        x_in[d] = go(send(tok, mine, xs.at[d - 1], xr.at[d - 1], at_x(d)))
    z_in = [[None] * 4, [None] * 4]
    z_in[0][0] = go(send(tok, mine, zs.at[0, 0], zr.at[0, 0], at_z(1)))
    z_in[1][0] = go(send(tok, mine, zs.at[1, 0], zr.at[1, 0], at_z(3)))
    d_in = [[None] * 4 for _ in range(4)]
    d_in[0][0] = go(send(tok, mine, ds.at[0, 0], dr.at[0, 0], mate))
    keep = pltpu.make_async_copy(tok, mine, own.at[0])
    keep.start()

    rows = pl.ds(pl.multiple_of(q * 512, 512), 512)
    l_in = [go(send(left, L.at[rows], ls.at[t], lr.at[t], group[t])) for t in range(3)]
    keep_l = pltpu.make_async_copy(left, L.at[rows], own.at[1])
    keep_l.start()

    def weight_copies(j):
        local, remote = [], []
        for g, w in enumerate((gate_w, up_w)):
            dst = W.at[j, rows, pl.ds(g * 128, 128)]
            for t in (1, 2, 0):
                cols = pl.ds(pl.multiple_of(group_q[t] * 896 + j * 128, 128), 128)
                remote.append(send(w.at[:, cols], dst, ws.at[j, g, t], wr.at[j, g, t], group[t]))
            cols = pl.ds(pl.multiple_of(q * 896 + j * 128, 128), 128)
            local.append(pltpu.make_async_copy(w.at[:, cols], dst, wl.at[j, g]))
        return local, remote

    def fetch(j):
        local, remote = weight_copies(j)
        for copy in remote + local:
            copy.start()


    for d in (1, 3, 2):
        x_in[d].wait_recv()
        here = tile(0, d)
        z_in[0][d] = go(send(here, here, zs.at[0, d], zr.at[0, d], at_z(1)))
        z_in[1][d] = go(send(here, here, zs.at[1, d], zr.at[1, d], at_z(3)))
        d_in[0][d] = go(send(here, here, ds.at[0, d], dr.at[0, d], mate))
    f_in = [[None] * 4, [None] * 4]
    for d in (0, 1, 3, 2):
        for s in range(2):
            z_in[s][d].wait_recv()
            dz = 3 if s == 0 else 1
            part = tile(dz, d, 128 * s, 128)
            f_in[s][d] = go(send(part, part, fs.at[s, d], fr.at[s, d], at_z(1 if s == 0 else 3)))
            here = tile(dz, d)
            d_in[1 + s][d] = go(send(here, here, ds.at[1 + s, d], dr.at[1 + s, d], mate))
        if d == 3:

            @pl.loop(0, 3)
            def _(j):
                fetch(j)

    for d in (0, 1, 3, 2):
        f_in[0][d].wait_recv()
        f_in[1][d].wait_recv()
        here = tile(2, d)
        d_in[3][d] = go(send(here, here, ds.at[3, d], dr.at[3, d], mate))

    @pl.loop(3, NJ)
    def _(j):
        fetch(j)

    keep.wait()
    keep_l.wait()
    for copy in l_in:
        copy.wait_recv()
    for i in range(4):
        for d in range(4):
            d_in[i][d].wait_recv()

    def partial(b, h, j):
        t = X[pl.ds(4 * h, 4), pl.ds(pl.multiple_of(b * 64, 64), 64), :].reshape(256, 2048)
        return jnp.dot(t, W[j], preferred_element_type=jnp.float32)

    def chain(j, h):
        return send(A_s.at[j, h], A_r.at[j, h], as_.at[j, h], ar.at[j, h], at_y(1 if h == 0 else 3))

    def direct(j, h):
        return send(B_s.at[j, h], B_r.at[j, h], bs.at[j, h], br.at[j, h], at_y(3 if h == 0 else 1))

    def last(j, h):
        return send(C_s.at[j, h], C_r.at[j, h], cs.at[j, h], cr.at[j, h], at_y(1 if h == 0 else 3))

    def squares(j):
        return [send(q_s.at[j], q_r.at[j, d - 1], qs.at[j, d - 1], qr.at[j, d - 1], at_y(d)) for d in (1, 2, 3)]

    def finish(j):
        for copy in squares(j):
            copy.wait_recv()
        sq = jnp.sum(q_s[j] + q_r[j, 0] + q_r[j, 1] + q_r[j, 2], axis=0, keepdims=True)
        cols = pl.ds(pl.multiple_of(q * 896 + j * 128, 128), 128)
        gate_scale = column_scale(gate_m[cols][None], sq[:, :128])
        up_scale = column_scale(up_m[cols][None], sq[:, 128:])
        for h in range(2):
            direct(j, h).wait_recv()
            last(j, h).wait_recv()
            total = partial(y, h, j) + B_r[j, h].astype(jnp.float32) + C_r[j, h].astype(jnp.float32)
            gate = total[:, :128] * gate_scale
            up = total[:, 128:] * up_scale
            value = gate / (1.0 + jnp.exp(-gate)) * up
            hid[pl.ds(4 * h, 4), :, pl.ds(pl.multiple_of(j * 128, 128), 128)] = value.astype(
                jnp.bfloat16
            ).reshape(4, 64, 128)

    @pl.loop(0, NJ)
    def _(j):
        local, remote = weight_copies(j)
        for copy in local:
            copy.wait()
        for copy in remote:
            copy.wait_recv()
        cols = pl.ds(pl.multiple_of(q * 896 + j * 128, 128), 128)
        zero = jnp.zeros((64, 128), jnp.bfloat16)
        right = jnp.concatenate(
            [
                jnp.concatenate([gate_r[:, cols], zero], axis=1),
                jnp.concatenate([zero, up_r[:, cols]], axis=1),
            ],
            axis=0,
        )
        q_s[j] = jnp.zeros((8, 256), jnp.float32)

        @pl.loop(0, 8)
        def _(i):
            part = pl.ds(pl.multiple_of(i * 256, 256), 256)
            merged = W[j, part].astype(jnp.float32) + jnp.dot(
                L[part], right, preferred_element_type=jnp.float32
            )
            q_s[j] += jnp.sum((merged * merged).reshape(32, 8, 256), axis=0)
            W[j, part] = merged.astype(jnp.bfloat16)

        for h in range(2):
            A_s[j, h] = partial((y + 2) % 4, h, j).astype(jnp.bfloat16)
            chain(j, h).start()
        for copy in squares(j):
            copy.start()
        for h in range(2):
            B_s[j, h] = partial((y + (3 if h == 0 else 1)) % 4, h, j).astype(jnp.bfloat16)
            direct(j, h).start()
        for h in range(2):
            value = partial((y + (1 if h == 0 else 3)) % 4, h, j)
            chain(j, h).wait_recv()
            C_s[j, h] = (value + A_r[j, h].astype(jnp.float32)).astype(jnp.bfloat16)
            last(j, h).start()

        @pl.when(j >= 1)
        def _():
            finish(j - 1)

    finish(NJ - 1)

    for copy in started:
        copy.wait_send()

    @pl.loop(0, NJ)
    def _(j):
        for copy in weight_copies(j)[1] + squares(j):
            copy.wait_send()
        for h in range(2):
            chain(j, h).wait_send()
            direct(j, h).wait_send()
            last(j, h).wait_send()


def hidden_of(tok, gate_w, up_w, left, gate_r, up_r, gate_m, up_m):
    anywhere = pl.BlockSpec(memory_space=pl.ANY)
    vmem = pl.BlockSpec(memory_space=pltpu.VMEM)
    dma = lambda *s: pltpu.SemaphoreType.DMA(s)
    piece = lambda: pltpu.VMEM((NJ, 2, 256, 256), jnp.bfloat16)
    return pl.pallas_call(
        hidden_kernel,
        out_shape=jax.ShapeDtypeStruct((8, 64, 896), jnp.bfloat16),
        in_specs=[anywhere, anywhere, anywhere, vmem, vmem, vmem, vmem, vmem],
        out_specs=vmem,
        scratch_shapes=[
            pltpu.VMEM((8, 256, 2048), jnp.bfloat16),
            pltpu.VMEM((NJ, 2048, 256), jnp.bfloat16),
            pltpu.VMEM((2048, 128), jnp.bfloat16),
            piece(), piece(), piece(), piece(), piece(), piece(),
            pltpu.VMEM((NJ, 8, 256), jnp.float32),
            pltpu.VMEM((NJ, 3, 8, 256), jnp.float32),
            dma(2), dma(3), dma(3), dma(2, 4), dma(2, 4), dma(2, 4), dma(2, 4), dma(4, 4), dma(4, 4),
            dma(NJ, 2), dma(NJ, 2, 3), dma(NJ, 2, 3), dma(3), dma(3),
            dma(NJ, 2), dma(NJ, 2), dma(NJ, 2), dma(NJ, 2), dma(NJ, 2), dma(NJ, 2),
            dma(NJ, 3), dma(NJ, 3),
        ],
        compiler_params=pltpu.CompilerParams(
            collective_id=0, has_side_effects=True, vmem_limit_bytes=60 * 2**20
        ),
        name="hidden_kernel",
    )(tok, gate_w, up_w, left, gate_r, up_r, gate_m, up_m)


def mix_kernel(
    hid, down_w, left, right, mag, out,
    H, W, R, M_s, M_r, F, G, A_s, B_s, C_s, A_r, B_r, C_r, D_s, D_r, sq, q_m, q_t, q_r,
    own, hs, hr, ys, yr, fs, fr, ws, wr, ms, mr, as_, ar, bs, br, cs, cr, ds, dr, qs, qr,
):
    z, xlo, y, xhi, core = place()

    def at(dz=0, dx=0, dy=0):
        return device((z + dz) % 4, (xlo + dx) % 2, (y + dy) % 4, xhi, core)

    mate = device(z, xlo, y, xhi, 1 - core)
    across = device(z, xlo, y, 1 - xhi, core)
    rows_peers = [(dz, dx) for dz in range(4) for dx in range(2)][1:]
    greet([mate, across, at(dy=1), at(dy=3)] + [at(dz=dz, dx=dx) for dz, dx in rows_peers])
    started = []

    def go(copy):
        copy.start()
        started.append(copy)
        return copy

    h_in = go(send(hid, H.at[y, xhi], hs.at[0], hr.at[0], across))
    y_in = [[None, None], [None, None]]
    for s in range(2):
        y_in[s][0] = go(send(hid, H.at[y, xhi], ys.at[s, 0], yr.at[s, 0], at(dy=1 if s == 0 else 3)))
    keep = pltpu.make_async_copy(hid, H.at[y, xhi], own.at[0])
    keep.start()

    w_in, w_own = [], []
    w_in.append(go(send(right, R.at[core], ws.at[2], wr.at[2], mate)))
    for xh in range(2):
        theirs = pl.ds(pl.multiple_of((xh * 2 + 1 - core) * 896, 128), 896)
        ours = pl.ds(pl.multiple_of((xh * 2 + core) * 896, 128), 896)
        w_in.append(go(send(down_w.at[theirs], W.at[core, xh], ws.at[xh], wr.at[xh], mate)))
        w_own.append(pltpu.make_async_copy(down_w.at[ours], W.at[core, xh], own.at[1 + xh]))
    w_own.append(pltpu.make_async_copy(right, R.at[core], own.at[3]))
    for copy in w_own:
        copy.start()
    for copy in w_own:
        copy.wait()
    for copy in w_in:
        copy.wait_recv()
    for cc in range(2):
        sq[cc] = jnp.zeros((8, 512), jnp.float32)
        for xh in range(2):

            @pl.loop(0, 7)
            def _(i):
                part = pl.ds(pl.multiple_of(i * 128, 128), 128)
                rows = pl.ds(pl.multiple_of((xh * 2 + core) * 896 + i * 128, 128), 128)
                merged = W[cc, xh, part].astype(jnp.float32) + jnp.dot(
                    left[rows], R[cc], preferred_element_type=jnp.float32
                )
                sq[cc] += jnp.sum((merged * merged).reshape(16, 8, 512), axis=0)
                W[cc, xh, part] = merged.astype(jnp.bfloat16)

    q_in = go(send(sq.at[1 - core], q_m, qs.at[7], qr.at[7], mate))
    q_in.wait_recv()
    q_t[...] = sq[core] + q_m[...]
    row_in = []
    for i, (dz, dx) in enumerate(rows_peers):
        row_in.append(go(send(q_t, q_r.at[i], qs.at[i], qr.at[i], at(dz=dz, dx=dx))))

    h_in.wait_recv()
    for s in range(2):
        block = H.at[y, 1 - xhi]
        y_in[s][1] = go(send(block, block, ys.at[s, 1], yr.at[s, 1], at(dy=1 if s == 0 else 3)))

    def pass_on(i):
        xh = xhi if i == 0 else 1 - xhi
        for s in range(2):
            y_in[s][i].wait_recv()
            part = H.at[(y + (3 if s == 0 else 1)) % 4, xh, pl.ds(4 * s, 4)]
            send(part, part, fs.at[s, i], fr.at[s, i], at(dy=1 if s == 0 else 3)).start()

    pass_on(0)
    keep.wait()
    for copy in row_in:
        copy.wait_recv()
    squares = q_t[...]
    for i in range(7):
        squares = squares + q_r[i]
    scale = column_scale(mag[...][None], jnp.sum(squares, axis=0, keepdims=True))

    def up_z(h):
        return at(dz=1 if h == 0 else 3)

    def down_z(h):
        return at(dz=3 if h == 0 else 1)

    def to_mate(i):
        return send(M_s.at[i], M_r.at[i], ms.at[i], mr.at[i], mate)

    def chain(i, h):
        return send(A_s.at[i, h], A_r.at[i, h], as_.at[i, h], ar.at[i, h], up_z(h))

    def direct(i, h):
        return send(B_s.at[i, h], B_r.at[i, h], bs.at[i, h], br.at[i, h], down_z(h))

    def last(i, h):
        return send(C_s.at[i, h], C_r.at[i, h], cs.at[i, h], cr.at[i, h], up_z(h))

    def aside(i):
        return send(D_s.at[i], D_r.at[i], ds.at[i], dr.at[i], at(dx=1))

    def block(i):
        b = (y + 3 * i + 3 * (i // 2) + 2 * (i // 3)) % 4

        def product(cc, n):
            cols = pl.ds(pl.multiple_of(n * 256, 256), 256)
            total = jnp.dot(
                H[b, 0].reshape(512, 896), W[cc, 0, :, cols], preferred_element_type=jnp.float32
            )
            return total + jnp.dot(
                H[b, 1].reshape(512, 896), W[cc, 1, :, cols], preferred_element_type=jnp.float32
            )

        @pl.loop(0, 2)
        def _(n):
            cols = pl.ds(pl.multiple_of(n * 256, 256), 256)
            M_s[i, :, cols] = product(1 - core, n).astype(jnp.bfloat16)

        to_mate(i).start()

        @pl.loop(0, 2)
        def _(n):
            cols = pl.ds(pl.multiple_of(n * 256, 256), 256)
            F[:, :, cols] = product(core, n).reshape(8, 64, 256)

        to_mate(i).wait_recv()
        F[...] += M_r[i].astype(jnp.float32).reshape(8, 64, 512)
        for h in range(2):
            A_s[i, h] = F[((z + 2) % 4) * 2 + h].astype(jnp.bfloat16)
            chain(i, h).start()
        for h in range(2):
            B_s[i, h] = F[((z + (3 if h == 0 else 1)) % 4) * 2 + h].astype(jnp.bfloat16)
            direct(i, h).start()
        for h in range(2):
            chain(i, h).wait_recv()
            value = F[((z + (1 if h == 0 else 3)) % 4) * 2 + h] + A_r[i, h].astype(jnp.float32)
            C_s[i, h] = value.astype(jnp.bfloat16)
            last(i, h).start()
        for h in range(2):
            direct(i, h).wait_recv()
            last(i, h).wait_recv()
            G[h] = F[z * 2 + h] + B_r[i, h].astype(jnp.float32) + C_r[i, h].astype(jnp.float32)
        D_s[i] = G[1 - xlo].astype(jnp.bfloat16)
        aside(i).start()
        aside(i).wait_recv()
        total = (G[xlo] + D_r[i].astype(jnp.float32)) * scale
        out[pl.ds(pl.multiple_of(b * 64, 64), 64), :] = total.astype(jnp.bfloat16)

    @pl.loop(0, 4)
    def _(i):
        @pl.when(i == 1)
        def _():
            pass_on(1)

        @pl.when(i == 3)
        def _():
            for s in range(2):
                for k in range(2):
                    part = H.at[(y + 2) % 4, (xhi, 1 - xhi)[k], pl.ds(4 * s, 4)]
                    send(part, part, fs.at[s, k], fr.at[s, k], at(dy=1 if s == 0 else 3)).wait_recv()

        block(i)

    for copy in started:
        copy.wait_send()
    for s in range(2):
        for k in range(2):
            part = H.at[(y + (3 if s == 0 else 1)) % 4, (xhi, 1 - xhi)[k], pl.ds(4 * s, 4)]
            send(part, part, fs.at[s, k], fr.at[s, k], at(dy=1 if s == 0 else 3)).wait_send()

    @pl.loop(0, 4)
    def _(i):
        to_mate(i).wait_send()
        aside(i).wait_send()
        for h in range(2):
            chain(i, h).wait_send()
            direct(i, h).wait_send()
            last(i, h).wait_send()


def mixed_of(hid, down_w, left, right, mag):
    anywhere = pl.BlockSpec(memory_space=pl.ANY)
    vmem = pl.BlockSpec(memory_space=pltpu.VMEM)
    dma = lambda *s: pltpu.SemaphoreType.DMA(s)
    bf = lambda *s: pltpu.VMEM(s, jnp.bfloat16)
    f32 = lambda *s: pltpu.VMEM(s, jnp.float32)
    piece = lambda: bf(4, 2, 64, 512)
    return pl.pallas_call(
        mix_kernel,
        out_shape=jax.ShapeDtypeStruct((256, 512), jnp.bfloat16),
        in_specs=[vmem, anywhere, vmem, vmem, vmem],
        out_specs=vmem,
        scratch_shapes=[
            bf(4, 2, 8, 64, 896), bf(2, 2, 896, 512), bf(2, 64, 512), bf(4, 512, 512), bf(4, 512, 512),
            f32(8, 64, 512), f32(2, 64, 512),
            piece(), piece(), piece(), piece(), piece(), piece(), bf(4, 64, 512), bf(4, 64, 512),
            f32(2, 8, 512), f32(8, 512), f32(8, 512), f32(7, 8, 512),
            dma(4), dma(1), dma(1), dma(2, 2), dma(2, 2), dma(2, 2), dma(2, 2), dma(3), dma(3),
            dma(4), dma(4), dma(4, 2), dma(4, 2), dma(4, 2), dma(4, 2), dma(4, 2), dma(4, 2),
            dma(4), dma(4), dma(8), dma(8),
        ],
        compiler_params=pltpu.CompilerParams(
            collective_id=1, has_side_effects=True, vmem_limit_bytes=60 * 2**20
        ),
        name="mix_kernel",
    )(hid, down_w, left, right, mag)


def shards(
    tokens,
    gate_frozen_weight, gate_left_factor, gate_right_factor, gate_column_magnitude,
    up_frozen_weight, up_left_factor, up_right_factor, up_column_magnitude,
    down_frozen_weight, down_left_factor, down_right_factor, down_column_magnitude,
):
    left = jnp.concatenate([gate_left_factor, up_left_factor], axis=1)
    hidden = hidden_of(
        tokens, gate_frozen_weight, up_frozen_weight, left, gate_right_factor, up_right_factor,
        gate_column_magnitude, up_column_magnitude,
    )
    return mixed_of(
        hidden, down_frozen_weight, down_left_factor, down_right_factor, down_column_magnitude
    )


def solution(mesh):
    placed = (
        P("row", "col"),
        P("col", "row"), P("col", None), P(None, "row"), P("row"),
        P("col", "row"), P("col", None), P(None, "row"), P("row"),
        P("row", "col"), P("row", None), P(None, "col"), P("col"),
    )
    return jax.shard_map(
        shards, mesh=mesh, in_specs=placed, out_specs=P("row", "col"), check_vma=False
    )
```
